32 devices in a mesh: inter: 16 (over z, y, core), intra: 2 (over x).
Axes of the slice: x: 2, y: 2, z: 4, core: 2. Of those that a mesh axis runs over, the one named last changes fastest.
Arguments:
- partials: bfloat16 [32, 16, 5120], P(('inter', 'intra')), may hold values from -6 to 6
- scales: bfloat16 [32, 16, 20], P(('inter', 'intra')), may hold values from 64 to 1024
- overflow_pos: int32 [32, 1], P(('inter', 'intra')), may hold values from -81920 to 81919, as said below
- weights: float32 [16, 5120], P('inter', 'intra'), may hold values from -6 to 6
- exponent: int32 [], replicated, may hold values from 10 to 16
Outputs:
- grad_out: float32 [16, 5120], P('inter', 'intra')
- block_scale: float32 [16, 20], P('inter', 'intra')
- master_out: float32 [16, 5120], P('inter', 'intra')
- new_exponent: int32 [], replicated
- overflow_count: int32 [], replicated
The draws below stay inside these ranges and needn't reach their ends.
Inputs may be any that keep to these rules, and one draw needn't show every extreme that they name: `overflow_pos`: A negative entry means no overflow on that device; otherwise it is the flat position (row times 5120 plus column) of an overflowed value of that device's partial.
All inputs are finite; a program needn't handle non-finite values.
Results may differ from the reference program's by a relative error of at most 0.0005.
Values may be sent and summed in bfloat16 or wider, within the bound.
A program may use at most 64 MiB of HBM per device.

```python
import math
import jax
import jax.numpy as jnp
from jax import lax

D = 5120
BLOCK = 256
ROWS = 16
N_INTRA = 2
DEVICES = 32


def draw_overflow_pos(key, part):
    key_lead, key_more, key_pos, key_neg, key_pick = jax.random.split(jax.random.fold_in(key, 71), 5)
    group_total = DEVICES // N_INTRA
    negative = jax.random.randint(key_neg, (DEVICES, 1), -(ROWS * D), 0, dtype=jnp.int32)
    picked_device = jax.random.randint(key_pick, (), 0, DEVICES, dtype=jnp.int32)
    lead_member = jax.random.randint(key_lead, (group_total,), 0, N_INTRA, dtype=jnp.int32)
    member = jnp.arange(DEVICES, dtype=jnp.int32) % N_INTRA
    is_lead = member == jnp.repeat(lead_member, N_INTRA)
    extra_flag = jax.random.randint(key_more, (DEVICES,), 0, 2, dtype=jnp.int32) == 1
    flagged = jnp.logical_or(is_lead, extra_flag)
    positive = jax.random.randint(key_pos, (DEVICES, 1), 0, ROWS * D, dtype=jnp.int32)
    values = jnp.where(flagged[:, None], positive, negative)
    values = values.at[picked_device, 0].set(jnp.where(is_lead[picked_device], values[picked_device, 0], -(ROWS * D)))
    top_group = picked_device // N_INTRA
    top_device = top_group * N_INTRA + lead_member[top_group]
    return values.at[top_device, 0].set(ROWS * D - 1)


def spiked(array, key, source, target, blocks, factor):
    def block_of(axis_at):
        return (jnp.arange(array.shape[axis_at]) // (array.shape[axis_at] // blocks)).reshape((-1,) + (1,) * (array.ndim - 1 - axis_at))

    first = jax.random.permutation(key, blocks)[block_of(target)]
    far = (block_of(target) + blocks // 2) % blocks
    return jnp.where((block_of(source) == first) | (block_of(source) == far), factor * array, array)


def level_of(rng, extent, shards, low, top_value):
    gain, own = 1.0, jax.random.fold_in(rng, 6)
    for axis_at, parts in shards:
        heights = jnp.exp(jax.random.uniform(jax.random.fold_in(own, axis_at), (parts,), jnp.float32, low / len(shards), top_value / len(shards)))
        gain = gain * jnp.repeat(heights, extent[axis_at] // parts).reshape([-1 if axis == axis_at else 1 for axis in range(len(extent))])
    return gain


def gaussian(stream_key, shape, spread, reach, cuts=(), kind=jnp.bfloat16):
    factor_of = level_of(stream_key, shape, cuts, -0.22, 0.18) if cuts else 1.0
    values = jax.random.normal(stream_key, shape, jnp.float32) * spread * factor_of
    return jnp.minimum(jnp.maximum(values, -reach), reach).astype(kind)


def bell_draw_with(own_key, shape, deviation, reach, cuts, heavy, held_as=jnp.bfloat16):
    entries = deviation * jax.random.normal(own_key, shape, jnp.float32)
    if cuts:
        entries = entries * level_of(own_key, shape, cuts, -0.22, 0.18)
    return jnp.clip(spiked(entries, jax.random.fold_in(own_key, 3), *heavy), -reach, reach).astype(held_as)


def setup_inputs(seed: int = 0) -> dict:
    key_of = jax.random.split(jax.random.key(seed), 6)
    partials = bell_draw_with(key_of[0], (DEVICES, ROWS, D), 1.0, 6.0, ((0, 32),), (0, 1, 16, 2.0))
    scales = jnp.clip(jnp.exp(math.log(1024.0) - 2.7725887 * jax.random.uniform(key_of[1], (DEVICES, ROWS, D // BLOCK), jnp.float32) ** level_of(key_of[1], (DEVICES, ROWS, D // BLOCK), ((0, 32),), -0.2, 0.2)), 64.0, 1024.0).astype(jnp.bfloat16)
    overflow_pos = draw_overflow_pos(jax.random.fold_in(key_of[5], 71), 0)
    weights = gaussian(key_of[3], (ROWS, D), 1.0, 6.0, ((0, 16), (1, 2)), jnp.float32)
    exponent = jax.random.randint(key_of[4], (), 10, 17).astype(jnp.int32)
    return dict(partials=partials, scales=scales, overflow_pos=overflow_pos, weights=weights, exponent=exponent)


def reference(partials, scales, overflow_pos, weights, exponent):
    def add_term(grad_acc, inputs):
        levels, block_scales = inputs
        scaled = levels.astype(jnp.float32).reshape(ROWS, D // BLOCK, BLOCK) * block_scales.astype(jnp.float32)[:, :, None]
        return grad_acc + scaled.reshape(ROWS, D), None

    grad_sum, _ = lax.scan(add_term, jnp.zeros((ROWS, D), jnp.float32), (partials, scales))
    flag_count = jnp.sum((overflow_pos >= 0).astype(jnp.int32))
    grad_out = grad_sum * jnp.exp2(-exponent.astype(jnp.float32))
    block_scale = jnp.max(jnp.abs(grad_out.reshape(ROWS, D // BLOCK, BLOCK)), axis=2) / 127.0
    master_out = jnp.where(flag_count == 0, weights - 0.5 * grad_out, weights)
    new_exponent = exponent - (flag_count > 0).astype(jnp.int32)
    return grad_out, block_scale, master_out, new_exponent, flag_count
```

```python
import functools

import jax
import jax.numpy as jnp
from jax import lax
from jax.experimental import pallas as pl
from jax.experimental.pallas import tpu as pltpu
from jax.sharding import PartitionSpec as P

LANES = 128
CORES = 2
LINES = 2
MOST_LAYERS = 8
PREPARE_FLOPS = 60000000
ROW_GROUP = 16
SOURCE_GROUP = 32


def exchange(inter_size, intra_size, block_len, x_ref, tail_ref, meta_ref, w_hbm,
             grad_ref, scale_ref, master_ref, whole_ref,
             w_ref, staged, outgoing, incoming,
             load_sem, own_sem, send_sem, recv_sem, upper_sem):
    total = inter_size * intra_size
    xv = x_ref.at[0]
    row_total, full_width = xv.shape
    share_cols = full_width // intra_size
    half = share_cols // 2
    tiles = half // LANES
    my_inter = lax.axis_index("inter")
    my_intra = lax.axis_index("intra")
    me = my_inter * intra_size + my_intra

    barrier = pltpu.get_barrier_semaphore()
    cores, lines = CORES, LINES
    layers = inter_size // (cores * lines)
    ordered = layers * cores * lines == inter_size and layers <= MOST_LAYERS
    place = (my_inter // (cores * lines), lax.rem(my_inter // cores, lines), my_intra)
    ends = (layers, lines, intra_size)
    my_core = lax.rem(my_inter, cores)

    def each_chip(lows, highs, visit):
        def along_z(z, carry):
            def along_y(y, carry):
                def along_x(x, carry):
                    visit(z, y, x)
                    return carry
                return lax.fori_loop(lows[2], highs[2], along_x, carry)
            return lax.fori_loop(lows[1], highs[1], along_y, carry)
        lax.fori_loop(lows[0], highs[0], along_z, 0)

    def signal(semaphore, inter, intra):
        pl.semaphore_signal(semaphore, inc=1, device_id=(inter, intra), device_id_type=pl.DeviceIdType.MESH)

    if ordered:
        def greet(z, y, x):
            for core in range(cores):
                signal(barrier, (z * lines + y) * cores + core, x)

        if True:
            each_chip(place, ends, greet)
    else:
        for n in range(total):
            signal(barrier, n // intra_size, n % intra_size)

    load = pltpu.make_async_copy(w_hbm, w_ref, load_sem)
    load.start()

    def stage(group, carry):
        rows = pl.ds(pl.multiple_of(group * ROW_GROUP, ROW_GROUP), ROW_GROUP)
        for b in range(intra_size):
            for h in range(2):
                staged[:, b, h, :] = xv[rows, pl.ds((b * 2 + h) * half, half)].astype(jnp.float32)
        outgoing[rows, :, :, pl.ds(0, half)] = staged[...].astype(jnp.bfloat16)
        outgoing[rows, :, :, pl.ds(half, LANES)] = tail_ref[rows]
        return carry

    if True:
        lax.fori_loop(0, row_total // ROW_GROUP, stage, 0)

    own = pltpu.make_async_copy(outgoing.at[my_inter, my_intra], incoming.at[me], own_sem)
    own.start()

    def send(to_inter, to_intra):
        pltpu.make_async_remote_copy(
            src_ref=outgoing.at[to_inter, to_intra],
            dst_ref=incoming.at[me],
            send_sem=send_sem,
            recv_sem=recv_sem,
            device_id=(to_inter, to_intra),
            device_id_type=pl.DeviceIdType.MESH,
        ).start()

    if ordered:
        past = tuple(at + 1 for at in place)

        def send_chip(z, y, x):
            for core in range(cores):
                to_inter = (z * lines + y) * cores + core

                @pl.when((to_inter != my_inter) | (x != my_intra))
                def _():
                    send(to_inter, x)

        def tell(z, y, x):
            @pl.when((z != place[0]) | (y != place[1]) | (x != place[2]))
            def _():
                offset = ((place[0] - z) * lines + place[1] - y) * intra_size + place[2] - x
                signal(upper_sem.at[offset], (z * lines + y) * cores + my_core, x)

        if True:
            pl.semaphore_wait(barrier, past[0] * past[1] * past[2] * cores)
        if True:
            each_chip((0, 0, 0), past, tell)
        if True:
            each_chip((0, 0, 0), past, send_chip)
        offsets = [(dz, dy, dx) for dz in range(layers) for dy in range(lines) for dx in range(intra_size)]
        for offset in sorted(offsets, key=lambda at: (sum(at), at))[1:]:
            inside = functools.reduce(jnp.logical_and, [at + d < end for at, d, end in zip(place, offset, ends)])

            @pl.when(inside)
            def _():
                pl.semaphore_wait(upper_sem.at[(offset[0] * lines + offset[1]) * intra_size + offset[2]], 1)
                lows = tuple(at + d if d else 0 for at, d in zip(place, offset))
                highs = tuple(at + d + 1 for at, d in zip(place, offset))
                each_chip(lows, highs, send_chip)
    else:
        pl.semaphore_wait(barrier, total)
        for n in range(total - 1):
            target = n + (n >= me).astype(jnp.int32)
            send(target // intra_size, lax.rem(target, intra_size))
    load.wait()
    exponent = meta_ref[0:1, 1:2]
    unscale = jnp.exp2(jnp.broadcast_to(-exponent.astype(jnp.float32), (1, LANES)))
    own.wait()
    others = incoming.at[pl.ds(0, total - 1)]
    if True:
        pltpu.make_async_copy(others, others, recv_sem).wait()

    def reduce(group, sums):
        sources = pl.ds(group * SOURCE_GROUP, SOURCE_GROUP)
        factors = incoming[sources, :, pl.ds(half, LANES)].astype(jnp.float32)
        added = [
            jnp.sum(incoming[sources, :, pl.ds(t * LANES, LANES)].astype(jnp.float32) * factors[:, :, t:t + 1], axis=0)
            for t in range(tiles)
        ]
        added.append(jnp.sum(factors, axis=0))
        return tuple(s + a for s, a in zip(sums, added))

    sums = tuple(jnp.zeros((2, LANES), jnp.float32) for _ in range(tiles + 1))
    if True:
        if total == SOURCE_GROUP:
            sums = reduce(0, sums)
        else:
            sums = lax.fori_loop(0, total // SOURCE_GROUP, reduce, sums)
    lane = lax.broadcasted_iota(jnp.int32, (1, LANES), 1)
    count = jnp.sum(jnp.where(lane == tiles, sums[tiles][0:1], 0.0)).astype(jnp.int32)
    blocks = share_cols // block_len
    per_block = block_len // LANES
    block_lane = lax.broadcasted_iota(jnp.int32, (1, blocks), 1)
    largest = jnp.zeros((1, blocks), jnp.float32)
    tops = []
    for h in range(2):
        for t in range(tiles):
            grad = sums[t][h:h + 1] * unscale
            columns = pl.ds(h * half + t * LANES, LANES)
            grad_ref[0:1, columns] = grad
            weights = w_ref[0:1, columns]
            master_ref[0:1, columns] = jnp.where(count == 0, weights - 0.5 * grad, weights)
            tops.append(jnp.abs(grad))
    for n in range(blocks):
        top = functools.reduce(jnp.maximum, tops[n * per_block:(n + 1) * per_block])
        largest = jnp.where(block_lane == n, jnp.max(top, axis=1, keepdims=True), largest)
    scale_ref[...] = largest / 127.0
    whole_ref[0:1, pl.ds(0, LANES)] = jnp.broadcast_to(exponent - jnp.where(count > 0, 1, 0), (1, LANES))
    whole_ref[0:1, pl.ds(LANES, LANES)] = jnp.full((1, LANES), count, jnp.int32)
    if True:
        pltpu.make_async_copy(others, others, send_sem).wait()


def prepare(intra_size, half, block_len, meta_ref, s_ref, tail_ref):
    block_total = s_ref.shape[2]
    tiles = half // LANES
    row_total = s_ref.shape[1]
    flag = meta_ref[0:1, 0:1].astype(jnp.float32)
    lane = lax.broadcasted_iota(jnp.int32, (row_total, LANES), 1)
    pick_block = lax.broadcasted_iota(jnp.int32, (block_total, LANES), 0)
    pick_lane = lax.broadcasted_iota(jnp.int32, (block_total, LANES), 1)
    parts = []
    for b in range(intra_size):
        for h in range(2):
            start = (b * 2 + h) * half
            hit = (pick_block == (start + pick_lane * LANES) // block_len) & (pick_lane < tiles)
            spread = jnp.dot(s_ref[0], hit.astype(jnp.float32).astype(jnp.bfloat16),
                             preferred_element_type=jnp.float32)
            parts.append(jnp.where(lane == tiles, flag, spread))
    tail_ref[...] = jnp.stack(parts, axis=1).reshape(tail_ref.shape).astype(jnp.bfloat16)


def gather_scalars(pos_ref, exp_ref, meta_ref):
    lane = lax.broadcasted_iota(jnp.int32, (1, LANES), 1)
    meta_ref[...] = jnp.where(lane == 0, jnp.where(pos_ref[0, 0] >= 0, 1, 0), exp_ref[...])


def finish(grad_in, scale_in, master_in, whole_in, grad_ref, scale_ref, master_ref, exp_ref, count_ref, exp_s, count_s, sems):
    copies = [
        pltpu.make_async_copy(src, dst, sems.at[n])
        for n, (src, dst) in enumerate(((grad_in, grad_ref), (scale_in, scale_ref), (master_in, master_ref)))
    ]
    for copy in copies:
        copy.start()
    exp_s[0] = whole_in[0:1, 0:1][0, 0]
    count_s[0] = whole_in[0:1, LANES:LANES + 1][0, 0]
    for n, (src, dst) in enumerate(((exp_s, exp_ref), (count_s, count_ref))):
        copies.append(pltpu.make_async_copy(src, dst, sems.at[3 + n]))
        copies[-1].start()
    for copy in copies:
        copy.wait()


def on_device(partials, scales, overflow_pos, weights, exponent):
    inter_size = lax.axis_size("inter")
    intra_size = lax.axis_size("intra")
    total = inter_size * intra_size
    row_total, full_width = partials.shape[1], partials.shape[2]
    block_total = scales.shape[2]
    block_len = full_width // block_total
    share_cols = full_width // intra_size
    blocks = share_cols // block_len
    width = share_cols // 2 + LANES
    any_space = pl.BlockSpec(memory_space=pl.ANY)
    vmem = pl.BlockSpec(memory_space=pltpu.VMEM)
    smem = pl.BlockSpec(memory_space=pltpu.SMEM)

    def in_vmem(array):
        return pltpu.with_memory_space_constraint(array, pltpu.VMEM)

    meta = pl.pallas_call(
        gather_scalars,
        out_shape=pltpu.VMEM((1, LANES), jnp.int32),
        in_specs=[smem, smem],
        out_specs=vmem,
        cost_estimate=pl.CostEstimate(flops=1000000, bytes_accessed=0, transcendentals=0),
        name="gather_scalars",
    )(overflow_pos, exponent)
    tails = pl.pallas_call(
        functools.partial(prepare, intra_size, width - LANES, block_len),
        out_shape=pltpu.VMEM((row_total, intra_size, 2, LANES), jnp.bfloat16),
        in_specs=[vmem, vmem],
        out_specs=vmem,
        cost_estimate=pl.CostEstimate(flops=PREPARE_FLOPS, bytes_accessed=0, transcendentals=0),
        name="prepare",
    )(in_vmem(meta), in_vmem(scales))
    results = pl.pallas_call(
        functools.partial(exchange, inter_size, intra_size, block_len),
        out_shape=(
            pltpu.VMEM((1, share_cols), jnp.float32),
            pltpu.VMEM((1, blocks), jnp.float32),
            pltpu.VMEM((1, share_cols), jnp.float32),
            pltpu.VMEM((1, 2 * LANES), jnp.int32),
        ),
        in_specs=[vmem, vmem, vmem, any_space],
        out_specs=(vmem, vmem, vmem, vmem),
        scratch_shapes=[
            pltpu.VMEM((1, share_cols), jnp.float32),
            pltpu.VMEM((ROW_GROUP, intra_size, 2, width - LANES), jnp.float32),
            pltpu.VMEM((row_total, intra_size, 2, width), jnp.bfloat16),
            pltpu.VMEM((total, 2, width), jnp.bfloat16),
            pltpu.SemaphoreType.DMA,
            pltpu.SemaphoreType.DMA,
            pltpu.SemaphoreType.DMA,
            pltpu.SemaphoreType.DMA,
            pltpu.SemaphoreType.REGULAR((total // CORES,)),
        ],
        compiler_params=pltpu.CompilerParams(collective_id=0, has_side_effects=True),
        name="exchange",
    )(in_vmem(partials), in_vmem(tails), in_vmem(meta), weights)
    grad_out, block_scale, master_out, new_exponent, count = pl.pallas_call(
        finish,
        out_shape=(
            jax.ShapeDtypeStruct((1, share_cols), jnp.float32),
            jax.ShapeDtypeStruct((1, blocks), jnp.float32),
            jax.ShapeDtypeStruct((1, share_cols), jnp.float32),
            jax.ShapeDtypeStruct((1,), jnp.int32),
            jax.ShapeDtypeStruct((1,), jnp.int32),
        ),
        in_specs=[vmem] * 4,
        out_specs=(any_space,) * 5,
        scratch_shapes=[pltpu.SMEM((1,), jnp.int32), pltpu.SMEM((1,), jnp.int32), pltpu.SemaphoreType.DMA((5,))],
        name="finish",
    )(*(pltpu.with_memory_space_constraint(result, pltpu.VMEM) for result in results))
    return grad_out, block_scale, master_out, new_exponent.reshape(()), count.reshape(())


def solution(mesh):
    placed = (
        P(("inter", "intra"), None, None),
        P(("inter", "intra"), None, None),
        P(("inter", "intra"), None),
        P("inter", "intra"),
        P(),
    )
    return jax.shard_map(
        on_device,
        mesh=mesh,
        in_specs=placed,
        out_specs=(P("inter", "intra"), P("inter", "intra"), P("inter", "intra"), P(), P()),
        check_vma=False,
    )
```

```python
import functools

import jax
import jax.numpy as jnp
from jax import lax
from jax.experimental import pallas as pl
from jax.experimental.pallas import tpu as pltpu
from jax.sharding import PartitionSpec as P

LANES = 128
CORES = 2
LINES = 2
MOST_LAYERS = 8
ROW_GROUP = 16
SOURCE_GROUP = 32
MESH = pl.DeviceIdType.MESH


def exchange(inter_size, intra_size, x_ref, s_ref, meta_ref, w_hbm,
             grad_ref, scale_ref, master_ref, whole_ref,
             w_ref, staged, outgoing, incoming,
             load_sem, own_sem, send_sem, recv_sems, told_sem):
    total = inter_size * intra_size
    row_total, full_width = x_ref.shape[1:]
    block_total = s_ref.shape[2]
    block_len = full_width // block_total
    share_cols = full_width // intra_size
    half = share_cols // 2
    tiles = half // LANES
    layers = inter_size // (CORES * LINES)
    ordered = layers * CORES * LINES == inter_size and layers & (layers - 1) == 0 and layers <= MOST_LAYERS
    my_inter = lax.axis_index("inter")
    my_intra = lax.axis_index("intra")
    me = my_inter * intra_size + my_intra
    my_core = lax.rem(my_inter, CORES)
    place = (my_inter // (CORES * LINES), lax.rem(my_inter // CORES, LINES), my_intra)
    past = tuple(at + 1 for at in place)
    ends = (layers, LINES, intra_size)
    barrier = pltpu.get_barrier_semaphore()

    def each_chip(lows, highs, visit):
        def along_z(z, carry):
            def along_y(y, carry):
                def along_x(x, carry):
                    visit(z, y, x)
                    return carry
                return lax.fori_loop(lows[2], highs[2], along_x, carry)
            return lax.fori_loop(lows[1], highs[1], along_y, carry)
        lax.fori_loop(lows[0], highs[0], along_z, 0)

    def inter_of(z, y, core):
        return (z * LINES + y) * CORES + core

    def signal(semaphore, inter, intra):
        pl.semaphore_signal(semaphore, inc=1, device_id=(inter, intra), device_id_type=MESH)

    def elsewhere(z, y, x):
        return (z != place[0]) | (y != place[1]) | (x != place[2])

    def send(to_inter, to_intra, group):
        pltpu.make_async_remote_copy(
            src_ref=outgoing.at[to_inter, to_intra],
            dst_ref=incoming.at[me],
            send_sem=send_sem,
            recv_sem=recv_sems.at[group],
            device_id=(to_inter, to_intra),
            device_id_type=MESH,
        ).start()

    if ordered:
        def greet(z, y, x):
            @pl.when(elsewhere(z, y, x))
            def _():
                for core in range(CORES):
                    signal(barrier, inter_of(z, y, core), x)

        each_chip(place, ends, greet)

        for core in range(CORES):
            @pl.when(core != my_core)
            def _():
                signal(barrier, inter_of(place[0], place[1], core), my_intra)
    else:
        for n in range(total):
            signal(barrier, n // intra_size, n % intra_size)
    load = pltpu.make_async_copy(w_hbm, w_ref, load_sem)
    load.start()

    flag = meta_ref[0:1, 0:1].astype(jnp.float32)
    shares = 2 * intra_size
    pick_block = lax.broadcasted_iota(jnp.int32, (block_total, shares * LANES), 0)
    pick = lax.broadcasted_iota(jnp.int32, (block_total, shares * LANES), 1)
    pick_lane = pick % LANES
    hit = (pick_block == (pick // LANES * tiles + pick_lane) * LANES // block_len) & (pick_lane < tiles)
    hit = hit.astype(jnp.float32).astype(jnp.bfloat16)
    lane = lax.broadcasted_iota(jnp.int32, (ROW_GROUP, LANES), 1)

    def stage(group, carry):
        rows = pl.ds(pl.multiple_of(group * ROW_GROUP, ROW_GROUP), ROW_GROUP)
        spread = jnp.dot(s_ref[0, rows, :], hit, preferred_element_type=jnp.float32)
        for n in range(shares):
            b, h = divmod(n, 2)
            staged[:, b, h, pl.ds(0, half)] = x_ref[0, rows, pl.ds(n * half, half)].astype(jnp.float32)
            staged[:, b, h, pl.ds(half, LANES)] = jnp.where(lane == tiles, flag, spread[:, n * LANES:(n + 1) * LANES])
        outgoing[rows] = staged[...].astype(jnp.bfloat16)
        return carry

    if row_total == ROW_GROUP:
        stage(0, 0)
    else:
        lax.fori_loop(0, row_total // ROW_GROUP, stage, 0)

    if ordered:
        def send_chip(z, y, x):
            for core in range(CORES):
                @pl.when(elsewhere(z, y, x) | (core != my_core))
                def _():
                    send(inter_of(z, y, core), x, z ^ place[0])

        def send_lower(z, y, x):
            @pl.when(elsewhere(z, y, x) & (z + y + x > 0))
            def _():
                for core in range(CORES):
                    send(inter_of(z, y, core), x, z ^ place[0])

        def tell(z, y, x):
            @pl.when(elsewhere(z, y, x))
            def _():
                steps = place[0] - z + place[1] - y + place[2] - x
                signal(told_sem.at[steps - 1], inter_of(z, y, my_core), x)

        below = past[0] * past[1] * past[2] * CORES - 1
        pl.semaphore_wait(barrier, below)
        @pl.when(place[0] + place[1] + place[2] > 0)
        def _():
            for core in range(CORES):
                send(core, 0, place[0])
        each_chip((0, 0, 0), past, tell)
        each_chip((0, 0, 0), past, send_lower)
        for core in range(CORES):
            @pl.when(core != my_core)
            def _():
                send(inter_of(place[0], place[1], core), my_intra, 0)

        offsets = [(dz, dy, dx) for dz in range(layers) for dy in range(LINES) for dx in range(intra_size)]
        for steps in range(1, sum(ends) - 2):
            level = [offset for offset in offsets if sum(offset) == steps]
            inside = [functools.reduce(jnp.logical_and, [at + d < end for at, d, end in zip(place, offset, ends)])
                      for offset in level]
            uppers = sum(each.astype(jnp.int32) for each in inside)

            @pl.when(uppers > 0)
            def _():
                pl.semaphore_wait(told_sem.at[steps - 1], uppers)

            for offset, each in zip(level, inside):
                @pl.when(each)
                def _():
                    lows = tuple(at + d if d else 0 for at, d in zip(place, offset))
                    highs = tuple(at + d + 1 for at, d in zip(place, offset))
                    each_chip(lows, highs, send_chip)

    else:
        pl.semaphore_wait(barrier, total)
        for n in range(total - 1):
            target = n + (n >= me).astype(jnp.int32)
            send(target // intra_size, lax.rem(target, intra_size), 0)

    own = pltpu.make_async_copy(outgoing.at[my_inter, my_intra], incoming.at[me], own_sem)
    own.start()
    exponent = meta_ref[0:1, 1:2]
    unscale = jnp.exp2(jnp.broadcast_to(-exponent.astype(jnp.float32), (1, LANES)))
    load.wait()
    own.wait()

    def add(first, size, sums):
        sources = pl.ds(first, size)
        factors = incoming[sources, :, pl.ds(half, LANES)].astype(jnp.float32)
        added = [
            jnp.sum(incoming[sources, :, pl.ds(t * LANES, LANES)].astype(jnp.float32) * factors[:, :, t:t + 1], axis=0)
            for t in range(tiles)
        ]
        added.append(jnp.sum(factors, axis=0))
        return tuple(s + a for s, a in zip(sums, added))

    def arrived(group, size):
        landed = incoming.at[pl.ds(0, size)]
        pltpu.make_async_copy(landed, landed, recv_sems.at[group]).wait()

    sums = tuple(jnp.zeros((2, LANES), jnp.float32) for _ in range(tiles + 1))
    if ordered:
        per_layer = total // layers
        for group in range(layers):
            arrived(group, per_layer - (group == 0))
            sums = add((place[0] ^ group) * per_layer, per_layer, sums)
    else:
        arrived(0, total - 1)
        sums = lax.fori_loop(0, total // SOURCE_GROUP, lambda n, sums: add(n * SOURCE_GROUP, SOURCE_GROUP, sums), sums)
    lane = lax.broadcasted_iota(jnp.int32, (1, LANES), 1)
    count = jnp.sum(jnp.where(lane == tiles, sums[tiles][0:1], 0.0), axis=1, keepdims=True).astype(jnp.int32)
    keep = jnp.broadcast_to(count, (1, LANES)) == 0
    per_block = block_len // LANES
    peaks = []
    grads = []
    for t in range(tiles):
        grad = sums[t] * unscale
        grads.append(grad)
        peaks.append(jnp.max(jnp.abs(grad), axis=1, keepdims=True))
    for h in range(2):
        for t in range(tiles):
            grad = grads[t][h:h + 1]
            columns = pl.ds(h * half + t * LANES, LANES)
            grad_ref[0:1, columns] = grad
            weights = w_ref[0:1, columns]
            master_ref[0:1, columns] = jnp.where(keep, weights - 0.5 * grad, weights)
    blocks = share_cols // block_len
    block_lane = lax.broadcasted_iota(jnp.int32, (1, blocks), 1)
    largest = jnp.zeros((1, blocks), jnp.float32)
    for n in range(blocks):
        parts = [divmod(n * per_block + k, tiles) for k in range(per_block)]
        top = functools.reduce(jnp.maximum, [peaks[t][h:h + 1] for h, t in parts])
        largest = jnp.where(block_lane == n, top, largest)
    scale_ref[...] = largest / 127.0
    whole_ref[0:1, pl.ds(0, LANES)] = jnp.broadcast_to(exponent - jnp.where(count > 0, 1, 0), (1, LANES))
    whole_ref[0:1, pl.ds(LANES, LANES)] = jnp.broadcast_to(count, (1, LANES))
    sent = incoming.at[pl.ds(0, total - 1)]
    pltpu.make_async_copy(sent, sent, send_sem).wait()


def gather_scalars(pos_ref, exp_ref, meta_ref):
    lane = lax.broadcasted_iota(jnp.int32, (1, LANES), 1)
    meta_ref[...] = jnp.where(lane == 0, jnp.where(pos_ref[0, 0] >= 0, 1, 0), exp_ref[...])


def pass_scales(meta_ref, s_ref, passed_ref):
    passed_ref[...] = s_ref[...]


def finish(grad_in, scale_in, master_in, whole_in, grad_ref, scale_ref, master_ref, exp_ref, count_ref, exp_s, count_s, sems):
    copies = [
        pltpu.make_async_copy(src, dst, sems.at[n])
        for n, (src, dst) in enumerate(((grad_in, grad_ref), (scale_in, scale_ref), (master_in, master_ref)))
    ]
    for copy in copies:
        copy.start()
    exp_s[0] = whole_in[0:1, 0:1][0, 0]
    count_s[0] = whole_in[0:1, LANES:LANES + 1][0, 0]
    for n, (src, dst) in enumerate(((exp_s, exp_ref), (count_s, count_ref))):
        copies.append(pltpu.make_async_copy(src, dst, sems.at[3 + n]))
        copies[-1].start()
    for copy in copies:
        copy.wait()


def on_device(partials, scales, overflow_pos, weights, exponent):
    inter_size = lax.axis_size("inter")
    intra_size = lax.axis_size("intra")
    total = inter_size * intra_size
    row_total, full_width = partials.shape[1], partials.shape[2]
    block_len = full_width // scales.shape[2]
    share_cols = full_width // intra_size
    blocks = share_cols // block_len
    width = share_cols // 2 + LANES
    layers = inter_size // (CORES * LINES)
    steps = layers + LINES + intra_size - 3
    groups = layers if layers <= MOST_LAYERS else 1
    any_space = pl.BlockSpec(memory_space=pl.ANY)
    vmem = pl.BlockSpec(memory_space=pltpu.VMEM)
    smem = pl.BlockSpec(memory_space=pltpu.SMEM)

    def in_vmem(array):
        return pltpu.with_memory_space_constraint(array, pltpu.VMEM)

    meta = pl.pallas_call(
        gather_scalars,
        out_shape=pltpu.VMEM((1, LANES), jnp.int32),
        in_specs=[smem, smem],
        out_specs=vmem,
        cost_estimate=pl.CostEstimate(flops=1000000, bytes_accessed=0, transcendentals=0),
        name="gather_scalars",
    )(overflow_pos, exponent)
    passed = pl.pallas_call(
        pass_scales,
        out_shape=pltpu.VMEM(scales.shape, scales.dtype),
        in_specs=[vmem, vmem],
        out_specs=vmem,
        cost_estimate=pl.CostEstimate(flops=60000000, bytes_accessed=0, transcendentals=0),
        name="pass_scales",
    )(in_vmem(meta), in_vmem(scales))
    results = pl.pallas_call(
        functools.partial(exchange, inter_size, intra_size),
        out_shape=(
            pltpu.VMEM((1, share_cols), jnp.float32),
            pltpu.VMEM((1, blocks), jnp.float32),
            pltpu.VMEM((1, share_cols), jnp.float32),
            pltpu.VMEM((1, 2 * LANES), jnp.int32),
        ),
        in_specs=[vmem, vmem, vmem, any_space],
        out_specs=(vmem, vmem, vmem, vmem),
        scratch_shapes=[
            pltpu.VMEM((1, share_cols), jnp.float32),
            pltpu.VMEM((ROW_GROUP, intra_size, 2, width), jnp.float32),
            pltpu.VMEM((row_total, intra_size, 2, width), jnp.bfloat16),
            pltpu.VMEM((total, 2, width), jnp.bfloat16),
            pltpu.SemaphoreType.DMA,
            pltpu.SemaphoreType.DMA,
            pltpu.SemaphoreType.DMA,
            pltpu.SemaphoreType.DMA((groups,)),
            pltpu.SemaphoreType.REGULAR((steps,)),
        ],
        compiler_params=pltpu.CompilerParams(collective_id=0, has_side_effects=True),
        name="exchange",
    )(in_vmem(partials), in_vmem(passed), in_vmem(meta), weights)
    grad_out, block_scale, master_out, new_exponent, count = pl.pallas_call(
        finish,
        out_shape=(
            jax.ShapeDtypeStruct((1, share_cols), jnp.float32),
            jax.ShapeDtypeStruct((1, blocks), jnp.float32),
            jax.ShapeDtypeStruct((1, share_cols), jnp.float32),
            jax.ShapeDtypeStruct((1,), jnp.int32),
            jax.ShapeDtypeStruct((1,), jnp.int32),
        ),
        in_specs=[vmem] * 4,
        out_specs=(any_space,) * 5,
        scratch_shapes=[pltpu.SMEM((1,), jnp.int32), pltpu.SMEM((1,), jnp.int32), pltpu.SemaphoreType.DMA((5,))],
        name="finish",
    )(*(in_vmem(result) for result in results))
    return grad_out, block_scale, master_out, new_exponent.reshape(()), count.reshape(())


def solution(mesh):
    placed = (
        P(("inter", "intra"), None, None),
        P(("inter", "intra"), None, None),
        P(("inter", "intra"), None),
        P("inter", "intra"),
        P(),
    )
    return jax.shard_map(
        on_device,
        mesh=mesh,
        in_specs=placed,
        out_specs=(P("inter", "intra"), P("inter", "intra"), P("inter", "intra"), P(), P()),
        check_vma=False,
    )
```

```python
import functools

import jax
import jax.numpy as jnp
from jax import lax
from jax.experimental import pallas as pl
from jax.experimental.pallas import tpu as pltpu
from jax.sharding import PartitionSpec as P

LANES = 128
CORES = 2
LINES = 2
MOST_LAYERS = 8
KEEPER = CORES - 1
TAIL = 128
ROW_GROUP = 8
SOURCE_GROUP = 32
MESH = pl.DeviceIdType.MESH


def layers_of(inter_size):
    layers = inter_size // (CORES * LINES)
    return layers, layers * CORES * LINES == inter_size and 1 < layers <= MOST_LAYERS


def exchange(inter_size, intra_size, block_len, x_ref, s_ref, meta_ref, w_hbm,
             grad_ref, scale_ref, master_ref, whole_ref,
             w_ref, staged, outgoing, incoming, layer_in, layer_sum, sum_in,
             load_sem, own_sem, send_sem, sum_send_sem, recv_sems, layer_sems, told_sem, mate_sem):
    total = inter_size * intra_size
    row_total, full_width = x_ref.shape[1:]
    share_cols = full_width // intra_size
    half = share_cols // 2
    tiles = half // LANES
    layers, ordered = layers_of(inter_size)
    per_layer = total // layers if ordered else total
    scale_tiles = block_len // LANES if half % block_len == 0 else 1
    scale_lanes = tiles // scale_tiles
    my_inter = lax.axis_index("inter")
    my_intra = lax.axis_index("intra")
    me = my_inter * intra_size + my_intra
    my_core = lax.rem(my_inter, CORES)
    place = (my_inter // (CORES * LINES), lax.rem(my_inter // CORES, LINES), my_intra)
    at_first = place[0] + place[1] + place[2] == 0
    past = tuple(at + 1 for at in place)
    ends = (layers, LINES, intra_size)
    barrier = pltpu.get_barrier_semaphore()

    def each_chip(lows, highs, visit):
        def along_z(z, carry):
            def along_y(y, carry):
                def along_x(x, carry):
                    visit(z, y, x)
                    return carry
                return lax.fori_loop(lows[2], highs[2], along_x, carry)
            return lax.fori_loop(lows[1], highs[1], along_y, carry)
        lax.fori_loop(lows[0], highs[0], along_z, 0)

    def inter_of(z, y, core):
        return (z * LINES + y) * CORES + core

    def signal(semaphore, inter, intra):
        pl.semaphore_signal(semaphore, inc=1, device_id=(inter, intra), device_id_type=MESH)

    def elsewhere(z, y, x):
        return (z != place[0]) | (y != place[1]) | (x != place[2])

    def send(to_inter, to_intra, group):
        pltpu.make_async_remote_copy(
            src_ref=outgoing.at[to_inter, to_intra],
            dst_ref=incoming.at[me],
            send_sem=send_sem,
            recv_sem=recv_sems.at[group],
            device_id=(to_inter, to_intra),
            device_id_type=MESH,
        ).start()

    if ordered:
        def greet(z, y, x):
            @pl.when(elsewhere(z, y, x))
            def _():
                signal(barrier, inter_of(z, y, KEEPER), x)
                for core in range(KEEPER):
                    pl.when(at_first)(functools.partial(signal, barrier, inter_of(z, y, core), x))

        each_chip(place, ends, greet)
        pl.when(my_core != KEEPER)(lambda: signal(barrier, inter_of(place[0], place[1], KEEPER), my_intra))
        for core in range(KEEPER):
            pl.when(at_first & (my_core == KEEPER))(
                functools.partial(signal, barrier, inter_of(place[0], place[1], core), my_intra))
    else:
        for n in range(total):
            signal(barrier, n // intra_size, n % intra_size)
    load = pltpu.make_async_copy(w_hbm, w_ref, load_sem)
    load.start()

    flag = meta_ref[0:1, 0:1].astype(jnp.float32)
    shares = 2 * intra_size
    lane = lax.broadcasted_iota(jnp.int32, (ROW_GROUP, TAIL), 1)
    flags = jnp.where(lane == scale_lanes, flag, 0.0)

    def stage(group, carry):
        rows = pl.ds(pl.multiple_of(group * ROW_GROUP, ROW_GROUP), ROW_GROUP)
        scale_rows = s_ref[0, rows, :]
        for n in range(shares):
            b, h = divmod(n, 2)
            if scale_tiles > 1:
                spread = pltpu.roll(scale_rows, (LANES - n * scale_lanes) % LANES, 1)[:, :TAIL]
                spread = jnp.where(lane < scale_lanes, spread, flags)
            else:
                spread = flags
                for t in range(tiles):
                    block = (n * tiles + t) * LANES // block_len
                    spread = jnp.where(lane == t, scale_rows[:, block:block + 1], spread)
            staged[:, b, h, pl.ds(0, half)] = x_ref[0, rows, pl.ds(n * half, half)].astype(jnp.float32)
            staged[:, b, h, pl.ds(half, TAIL)] = spread
        outgoing[rows] = staged[...].astype(jnp.bfloat16)
        return carry

    stage(0, 0)

    def stage_rest():
        if row_total == 2 * ROW_GROUP:
            stage(1, 0)
        else:
            lax.fori_loop(1, row_total // ROW_GROUP, stage, 0)

    if ordered:
        flat = LINES + intra_size - 2
        my_slot = lax.rem(me, per_layer)

        def send_chip(z, y, x):
            for core in range(CORES):
                send(inter_of(z, y, core), x, place[0] - z)

        def send_other(z, y, x):
            pl.when(elsewhere(z, y, x) & (z + y + x > 0))(lambda: send_chip(z, y, x))

        def send_above(z, y, x, core):
            for up in range(1, layers):
                @pl.when(z + up < layers)
                def _():
                    pltpu.make_async_remote_copy(
                        src_ref=outgoing.at[inter_of(z + up, y, core), x],
                        dst_ref=layer_in.at[up - 1, my_slot],
                        send_sem=send_sem,
                        recv_sem=layer_sems.at[up - 1],
                        device_id=(inter_of(z, y, core), x),
                        device_id_type=MESH,
                    ).start()

        def send_chip_above(z, y, x):
            @pl.when(elsewhere(z, y, x))
            def _():
                for core in range(CORES):
                    send_above(z, y, x, core)

        def tell_flat(z, y, x):
            @pl.when(elsewhere(z, y, x))
            def _():
                signal(told_sem.at[place[1] - y + place[2] - x - 1], inter_of(z, y, my_core), x)

        def tell_down(z, y, x):
            @pl.when(elsewhere(z, y, x))
            def _():
                signal(told_sem.at[flat + place[0] - z - 1], inter_of(z, y, my_core), x)

        keeps = my_core == KEEPER
        below = past[0] * past[1] * past[2] * CORES - CORES
        pl.when(keeps)(stage_rest)
        pl.semaphore_wait(barrier, jnp.where(keeps, below + KEEPER, jnp.where(at_first, 1, CORES)))
        pl.when(~at_first)(lambda: send_chip(0, 0, 0))
        pl.when(~keeps)(stage_rest)
        for core in range(KEEPER):
            pl.when(keeps)(functools.partial(signal, mate_sem, inter_of(place[0], place[1], core), my_intra))
        pl.when(~keeps)(lambda: pl.semaphore_wait(mate_sem, 1))
        each_chip((place[0], 0, 0), past, tell_flat)
        each_chip((0, place[1], place[2]), past, tell_down)
        each_chip((0, 0, 0), past, send_other)
        each_chip((place[0], 0, 0), past, send_chip_above)
        for core in range(CORES):
            @pl.when(core != my_core)
            def _():
                send(inter_of(place[0], place[1], core), my_intra, 0)
                send_above(*place, core)

        offsets = [(dy, dx) for dy in range(LINES) for dx in range(intra_size)]
        for steps in range(1, flat + 1):
            level = [(0, *offset) for offset in offsets if sum(offset) == steps]
            inside = [functools.reduce(jnp.logical_and, [at + d < end for at, d, end in zip(place, offset, ends)])
                      for offset in level]
            uppers = sum(each.astype(jnp.int32) for each in inside)

            @pl.when(uppers > 0)
            def _():
                pl.semaphore_wait(told_sem.at[steps - 1], uppers)

            for offset, each in zip(level, inside):
                @pl.when(each)
                def _():
                    lows = tuple(at + d if d else 0 for at, d in zip(place, offset))
                    highs = tuple(at + d + 1 for at, d in zip(place, offset))
                    each_chip((place[0], *lows[1:]), highs, send_chip_above)
                    each_chip(lows, highs, send_chip)
    else:
        stage_rest()
        pl.semaphore_wait(barrier, total)
        for n in range(total - 1):
            target = n + (n >= me).astype(jnp.int32)
            send(target // intra_size, lax.rem(target, intra_size), 0)

    own = pltpu.make_async_copy(outgoing.at[my_inter, my_intra], incoming.at[me], own_sem)
    own.start()
    exponent = meta_ref[0:1, 1:2]
    unscale = jnp.exp2(jnp.broadcast_to(-exponent.astype(jnp.float32), (1, LANES)))
    load.wait()
    own.wait()

    def add(ref, sources, sums):
        factors = ref[sources, :, pl.ds(half, TAIL)].astype(jnp.float32)
        spread = [jnp.broadcast_to(factors[:, :, n:n + 1], (*factors.shape[:2], LANES)) for n in range(scale_lanes)]
        added = [
            jnp.sum(ref[sources, :, pl.ds(t * LANES, LANES)].astype(jnp.float32) * spread[t // scale_tiles], axis=0)
            for t in range(tiles)
        ]
        added.append(jnp.sum(factors, axis=0))
        return tuple(s + a for s, a in zip(sums, added))

    def landed(ref, semaphore):
        pltpu.make_async_copy(ref, ref, semaphore).wait()

    sums = tuple(jnp.zeros((2, LANES), jnp.float32) for _ in range(tiles)) + (jnp.zeros((2, TAIL), jnp.float32),)
    none = sums
    if ordered:
        for up in reversed(range(1, layers)):
            @pl.when(place[0] + up < layers)
            def _():
                mine = pltpu.make_async_copy(
                    outgoing.at[inter_of(place[0] + up, place[1], my_core), my_intra], layer_in.at[up - 1, my_slot], own_sem)
                mine.start()
                mine.wait()
                landed(layer_in.at[up - 1, pl.ds(0, per_layer - 1)], layer_sems.at[up - 1])
                for t, each in enumerate(add(layer_in.at[up - 1], pl.ds(0, per_layer), none)):
                    layer_sum[up - 1, :, pl.ds(t * LANES, each.shape[1])] = each
                pl.semaphore_wait(told_sem.at[flat + up - 1], 1)
                pltpu.make_async_remote_copy(
                    src_ref=layer_sum.at[up - 1],
                    dst_ref=sum_in.at[up - 1],
                    send_sem=sum_send_sem,
                    recv_sem=recv_sems.at[layers - up],
                    device_id=(inter_of(place[0] + up, place[1], my_core), my_intra),
                    device_id_type=MESH,
                ).start()

        landed(incoming.at[pl.ds(0, per_layer - 1)], recv_sems.at[0])
        sums = add(incoming, pl.ds(place[0] * per_layer, per_layer), sums)
        for group in range(1, layers):
            def direct(sums, group=group):
                landed(incoming.at[pl.ds(0, per_layer)], recv_sems.at[group])
                return add(incoming, pl.ds((place[0] + group) * per_layer, per_layer), sums)

            def summed(sums, group=group):
                below = sum_in.at[layers - group - 1]
                landed(below, recv_sems.at[group])
                return tuple(each + below[:, pl.ds(t * LANES, each.shape[1])] for t, each in enumerate(sums))

            sums = lax.cond(place[0] + group < layers, direct, summed, sums)
    else:
        landed(incoming.at[pl.ds(0, total - 1)], recv_sems.at[0])
        sums = lax.fori_loop(
            0, total // SOURCE_GROUP, lambda n, sums: add(incoming, pl.ds(n * SOURCE_GROUP, SOURCE_GROUP), sums), sums)
    lane = lax.broadcasted_iota(jnp.int32, (1, TAIL), 1)
    count = jnp.sum(jnp.where(lane == scale_lanes, sums[tiles][0:1], 0.0), axis=1, keepdims=True).astype(jnp.int32)
    keep = jnp.broadcast_to(count, (1, LANES)) == 0
    per_block = block_len // LANES
    peaks = []
    grads = []
    for t in range(tiles):
        grad = sums[t] * unscale
        grads.append(grad)
        peaks.append(jnp.max(jnp.abs(grad), axis=1, keepdims=True))
    for h in range(2):
        for t in range(tiles):
            grad = grads[t][h:h + 1]
            columns = pl.ds(h * half + t * LANES, LANES)
            grad_ref[0:1, columns] = grad
            weights = w_ref[0:1, columns]
            master_ref[0:1, columns] = jnp.where(keep, weights - 0.5 * grad, weights)
    blocks = share_cols // block_len
    block_lane = lax.broadcasted_iota(jnp.int32, (1, blocks), 1)
    largest = jnp.zeros((1, blocks), jnp.float32)
    for n in range(blocks):
        parts = [divmod(n * per_block + k, tiles) for k in range(per_block)]
        top = functools.reduce(jnp.maximum, [peaks[t][h:h + 1] for h, t in parts])
        largest = jnp.where(block_lane == n, top, largest)
    scale_ref[...] = largest / 127.0
    whole_ref[0:1, pl.ds(0, LANES)] = jnp.broadcast_to(exponent - jnp.where(count > 0, 1, 0), (1, LANES))
    whole_ref[0:1, pl.ds(LANES, LANES)] = jnp.broadcast_to(count, (1, LANES))
    def sent(layer):
        above = layers - 1 - layer
        landed(incoming.at[pl.ds(0, per_layer * (layer + 1) - 1 + (per_layer - 1) * above)], send_sem)
        if above:
            landed(layer_sum.at[pl.ds(0, above)], sum_send_sem)

    if ordered:
        for layer in range(layers):
            pl.when(place[0] == layer)(functools.partial(sent, layer))
    else:
        landed(incoming.at[pl.ds(0, total - 1)], send_sem)


def gather_scalars(pos_ref, exp_ref, meta_ref):
    lane = lax.broadcasted_iota(jnp.int32, (1, LANES), 1)
    meta_ref[...] = jnp.where(lane == 0, jnp.where(pos_ref[0, 0] >= 0, 1, 0), exp_ref[...])


def pass_scales(meta_ref, s_ref, passed_ref):
    passed_ref[0, :, pl.ds(0, s_ref.shape[2])] = s_ref[0].astype(jnp.float32)


def finish(grad_in, scale_in, master_in, whole_in, grad_ref, scale_ref, master_ref, exp_ref, count_ref, exp_s, count_s, sems):
    copies = [
        pltpu.make_async_copy(src, dst, sems.at[n])
        for n, (src, dst) in enumerate(((grad_in, grad_ref), (scale_in, scale_ref), (master_in, master_ref)))
    ]
    for copy in copies:
        copy.start()
    exp_s[0] = whole_in[0:1, 0:1][0, 0]
    count_s[0] = whole_in[0:1, LANES:LANES + 1][0, 0]
    for n, (src, dst) in enumerate(((exp_s, exp_ref), (count_s, count_ref))):
        copies.append(pltpu.make_async_copy(src, dst, sems.at[3 + n]))
        copies[-1].start()
    for copy in copies:
        copy.wait()


def on_device(partials, scales, overflow_pos, weights, exponent):
    inter_size = lax.axis_size("inter")
    intra_size = lax.axis_size("intra")
    total = inter_size * intra_size
    row_total, full_width = partials.shape[1], partials.shape[2]
    block_len = full_width // scales.shape[2]
    share_cols = full_width // intra_size
    blocks = share_cols // block_len
    width = share_cols // 2 + TAIL
    layers, ordered = layers_of(inter_size)
    groups, aboves, per_layer = (layers, layers - 1, total // layers) if ordered else (1, 1, 1)
    any_space = pl.BlockSpec(memory_space=pl.ANY)
    vmem = pl.BlockSpec(memory_space=pltpu.VMEM)
    smem = pl.BlockSpec(memory_space=pltpu.SMEM)

    def in_vmem(array):
        return pltpu.with_memory_space_constraint(array, pltpu.VMEM)

    meta = pl.pallas_call(
        gather_scalars,
        out_shape=pltpu.VMEM((1, LANES), jnp.int32),
        in_specs=[smem, smem],
        out_specs=vmem,
        cost_estimate=pl.CostEstimate(flops=1000000, bytes_accessed=0, transcendentals=0),
        name="gather_scalars",
    )(overflow_pos, exponent)
    passed = pl.pallas_call(
        pass_scales,
        out_shape=pltpu.VMEM((1, row_total, LANES), jnp.float32),
        in_specs=[vmem, vmem],
        out_specs=vmem,
        cost_estimate=pl.CostEstimate(flops=60000000, bytes_accessed=0, transcendentals=0),
        name="pass_scales",
    )(in_vmem(meta), in_vmem(scales))
    results = pl.pallas_call(
        functools.partial(exchange, inter_size, intra_size, block_len),
        out_shape=(
            pltpu.VMEM((1, share_cols), jnp.float32),
            pltpu.VMEM((1, blocks), jnp.float32),
            pltpu.VMEM((1, share_cols), jnp.float32),
            pltpu.VMEM((1, 2 * LANES), jnp.int32),
        ),
        in_specs=[vmem, vmem, vmem, any_space],
        out_specs=(vmem, vmem, vmem, vmem),
        scratch_shapes=[
            pltpu.VMEM((1, share_cols), jnp.float32),
            pltpu.VMEM((ROW_GROUP, intra_size, 2, width), jnp.float32),
            pltpu.VMEM((row_total, intra_size, 2, width), jnp.bfloat16),
            pltpu.VMEM((total, 2, width), jnp.bfloat16),
            pltpu.VMEM((aboves, per_layer, 2, width), jnp.bfloat16),
            pltpu.VMEM((aboves, 2, width), jnp.float32),
            pltpu.VMEM((aboves, 2, width), jnp.float32),
            pltpu.SemaphoreType.DMA,
            pltpu.SemaphoreType.DMA,
            pltpu.SemaphoreType.DMA,
            pltpu.SemaphoreType.DMA,
            pltpu.SemaphoreType.DMA((groups,)),
            pltpu.SemaphoreType.DMA((aboves,)),
            pltpu.SemaphoreType.REGULAR((LINES + intra_size - 2 + aboves,)),
            pltpu.SemaphoreType.REGULAR,
        ],
        compiler_params=pltpu.CompilerParams(collective_id=0, has_side_effects=True),
        name="exchange",
    )(in_vmem(partials), in_vmem(passed), in_vmem(meta), weights)
    grad_out, block_scale, master_out, new_exponent, count = pl.pallas_call(
        finish,
        out_shape=(
            jax.ShapeDtypeStruct((1, share_cols), jnp.float32),
            jax.ShapeDtypeStruct((1, blocks), jnp.float32),
            jax.ShapeDtypeStruct((1, share_cols), jnp.float32),
            jax.ShapeDtypeStruct((1,), jnp.int32),
            jax.ShapeDtypeStruct((1,), jnp.int32),
        ),
        in_specs=[vmem] * 4,
        out_specs=(any_space,) * 5,
        scratch_shapes=[pltpu.SMEM((1,), jnp.int32), pltpu.SMEM((1,), jnp.int32), pltpu.SemaphoreType.DMA((5,))],
        name="finish",
    )(*(in_vmem(result) for result in results))
    return grad_out, block_scale, master_out, new_exponent.reshape(()), count.reshape(())


def solution(mesh):
    placed = (
        P(("inter", "intra"), None, None),
        P(("inter", "intra"), None, None),
        P(("inter", "intra"), None),
        P("inter", "intra"),
        P(),
    )
    return jax.shard_map(
        on_device,
        mesh=mesh,
        in_specs=placed,
        out_specs=(P("inter", "intra"), P("inter", "intra"), P("inter", "intra"), P(), P()),
        check_vma=False,
    )
```

```python
import functools

import jax
import jax.numpy as jnp
from jax import lax
from jax.experimental import pallas as pl
from jax.experimental.pallas import tpu as pltpu
from jax.sharding import PartitionSpec as P

LANES = 128
CORES = 2
LINES = 2
MOST_LAYERS = 8
KEEPER = CORES - 1
TAIL = 128
ROW_GROUP = 8
SOURCE_GROUP = 32
MESH = pl.DeviceIdType.MESH


def layers_of(inter_size):
    layers = inter_size // (CORES * LINES)
    return layers, layers * CORES * LINES == inter_size and 1 < layers <= MOST_LAYERS


def exchange(inter_size, intra_size, block_len, x_ref, s_ref, meta_ref, w_hbm,
             grad_ref, scale_ref, master_ref, exp_ref, count_ref,
             w_ref, staged, outgoing, incoming, layer_in, layer_sum, sum_in,
             load_sem, send_sem, sum_send_sem, recv_sems, layer_sem, told_sem, mate_sem):
    total = inter_size * intra_size
    row_total, full_width = x_ref.shape[1:]
    share_cols = full_width // intra_size
    half = share_cols // 2
    tiles = half // LANES
    layers, ordered = layers_of(inter_size)
    per_layer = total // layers if ordered else total
    scale_tiles = block_len // LANES if half % block_len == 0 else 1
    scale_lanes = tiles // scale_tiles
    my_inter = lax.axis_index("inter")
    my_intra = lax.axis_index("intra")
    me = my_inter * intra_size + my_intra
    my_core = lax.rem(my_inter, CORES)
    place = (my_inter // (CORES * LINES), lax.rem(my_inter // CORES, LINES), my_intra)
    at_first = place[0] + place[1] + place[2] == 0
    past = tuple(at + 1 for at in place)
    ends = (layers, LINES, intra_size)
    barrier = pltpu.get_barrier_semaphore()

    def each_chip(lows, highs, visit):
        def along_z(z, carry):
            def along_y(y, carry):
                def along_x(x, carry):
                    visit(z, y, x)
                    return carry
                return lax.fori_loop(lows[2], highs[2], along_x, carry)
            return lax.fori_loop(lows[1], highs[1], along_y, carry)
        lax.fori_loop(lows[0], highs[0], along_z, 0)

    def inter_of(z, y, core):
        return (z * LINES + y) * CORES + core

    def signal(semaphore, inter, intra):
        pl.semaphore_signal(semaphore, inc=1, device_id=(inter, intra), device_id_type=MESH)

    def elsewhere(z, y, x):
        return (z != place[0]) | (y != place[1]) | (x != place[2])

    def send(to_inter, to_intra, group):
        pltpu.make_async_remote_copy(
            src_ref=outgoing.at[to_inter, to_intra],
            dst_ref=incoming.at[me],
            send_sem=send_sem,
            recv_sem=recv_sems.at[group],
            device_id=(to_inter, to_intra),
            device_id_type=MESH,
        ).start()

    if ordered:
        def greet(z, y, x):
            @pl.when(elsewhere(z, y, x))
            def _():
                signal(barrier, inter_of(z, y, KEEPER), x)
                for core in range(KEEPER):
                    pl.when(at_first)(functools.partial(signal, barrier, inter_of(z, y, core), x))

        each_chip(place, ends, greet)
        pl.when(my_core != KEEPER)(lambda: signal(barrier, inter_of(place[0], place[1], KEEPER), my_intra))
        for core in range(KEEPER):
            pl.when(at_first & (my_core == KEEPER))(
                functools.partial(signal, barrier, inter_of(place[0], place[1], core), my_intra))
    else:
        for n in range(total):
            signal(barrier, n // intra_size, n % intra_size)
    load = pltpu.make_async_copy(w_hbm, w_ref, load_sem)
    load.start()

    flag = meta_ref[0:1, 0:1].astype(jnp.float32)
    lane = lax.broadcasted_iota(jnp.int32, (ROW_GROUP, TAIL), 1)
    flags = jnp.where(lane == scale_lanes, flag, 0.0)

    def stage(group, shares):
        rows = pl.ds(pl.multiple_of(group * ROW_GROUP, ROW_GROUP), ROW_GROUP)
        scale_rows = s_ref[0, rows, :]
        for b in shares:
            for h in range(2):
                n = b * 2 + h
                if scale_tiles > 1:
                    spread = pltpu.roll(scale_rows, (LANES - n * scale_lanes) % LANES, 1)[:, :TAIL]
                    spread = jnp.where(lane < scale_lanes, spread, flags)
                else:
                    spread = flags
                    for t in range(tiles):
                        block = (n * tiles + t) * LANES // block_len
                        spread = jnp.where(lane == t, scale_rows[:, block:block + 1], spread)
                staged[:, b, h, pl.ds(0, half)] = x_ref[0, rows, pl.ds(n * half, half)].astype(jnp.float32)
                staged[:, b, h, pl.ds(half, TAIL)] = spread
            outgoing[rows, b] = staged[:, b].astype(jnp.bfloat16)

    stage(0, range(1))

    def stage_rest():
        stage(0, range(1, intra_size))
        if row_total == 2 * ROW_GROUP:
            stage(1, range(intra_size))
        else:
            lax.fori_loop(1, row_total // ROW_GROUP, lambda n, carry: (stage(n, range(intra_size)), carry)[1], 0)

    if ordered:
        flat = LINES + intra_size - 2
        my_slot = lax.rem(me, per_layer)

        def send_chip(z, y, x, cores=tuple(reversed(range(CORES)))):
            for core in cores:
                send(inter_of(z, y, core), x, place[0] - z)

        def send_planes(lows, highs, keep):
            def along(z, carry):
                for core in reversed(range(CORES)):
                    def visit(z, y, x):
                        pl.when(keep(z, y, x))(lambda: send_chip(z, y, x, (core,)))
                    each_chip((z, *lows[1:]), (z + 1, *highs[1:]), visit)
                return carry
            lax.fori_loop(lows[0], highs[0], along, 0)

        def send_above(z, y, x, core):
            for up in range(1, layers):
                @pl.when(z + up < layers)
                def _():
                    pltpu.make_async_remote_copy(
                        src_ref=outgoing.at[inter_of(z + up, y, core), x],
                        dst_ref=layer_in.at[up - 1, my_slot],
                        send_sem=send_sem,
                        recv_sem=layer_sem,
                        device_id=(inter_of(z, y, core), x),
                        device_id_type=MESH,
                    ).start()

        def send_chip_above(z, y, x):
            @pl.when(elsewhere(z, y, x))
            def _():
                for core in range(CORES):
                    send_above(z, y, x, core)

        def tell_flat(z, y, x):
            @pl.when(elsewhere(z, y, x))
            def _():
                signal(told_sem.at[place[1] - y + place[2] - x - 1], inter_of(z, y, my_core), x)

        def tell_down(z, y, x):
            @pl.when(elsewhere(z, y, x))
            def _():
                signal(told_sem.at[flat], inter_of(z, y, my_core), x)

        keeps = my_core == KEEPER
        below = past[0] * past[1] * past[2] * CORES - CORES
        pl.when(keeps)(stage_rest)
        pl.semaphore_wait(barrier, jnp.where(keeps, below + KEEPER, jnp.where(at_first, 1, CORES)))
        pl.when(~at_first)(lambda: send_chip(0, 0, 0, tuple(range(CORES))))
        pl.when(~keeps)(stage_rest)
        for core in range(KEEPER):
            pl.when(keeps)(functools.partial(signal, mate_sem, inter_of(place[0], place[1], core), my_intra))
        pl.when(~keeps)(lambda: pl.semaphore_wait(mate_sem, 1))
        each_chip((place[0], 0, 0), past, tell_flat)
        each_chip((0, place[1], place[2]), past, tell_down)
        send_planes((0, 0, 0), past, lambda z, y, x: elsewhere(z, y, x) & (z + y + x > 0))
        each_chip((place[0], 0, 0), past, send_chip_above)
        for core in range(CORES):
            @pl.when(core != my_core)
            def _():
                send(inter_of(place[0], place[1], core), my_intra, 0)
                send_above(*place, core)

        offsets = [(dy, dx) for dy in range(LINES) for dx in range(intra_size)]
        for steps in range(1, flat + 1):
            level = [(0, *offset) for offset in offsets if sum(offset) == steps]
            inside = [functools.reduce(jnp.logical_and, [at + d < end for at, d, end in zip(place, offset, ends)])
                      for offset in level]
            uppers = sum(each.astype(jnp.int32) for each in inside)

            @pl.when(uppers > 0)
            def _():
                pl.semaphore_wait(told_sem.at[steps - 1], uppers)

            for offset, each in zip(level, inside):
                @pl.when(each)
                def _():
                    lows = tuple(at + d if d else 0 for at, d in zip(place, offset))
                    highs = tuple(at + d + 1 for at, d in zip(place, offset))
                    each_chip((place[0], *lows[1:]), highs, send_chip_above)
                    send_planes(lows, highs, lambda z, y, x: True)
    else:
        stage_rest()
        pl.semaphore_wait(barrier, total)
        for n in range(total - 1):
            target = n + (n >= me).astype(jnp.int32)
            send(target // intra_size, lax.rem(target, intra_size), 0)

    incoming[me] = outgoing[my_inter, my_intra]
    exponent = meta_ref[0:1, 1:2]
    unscale = jnp.exp2(jnp.broadcast_to(-exponent.astype(jnp.float32), (1, LANES)))
    load.wait()

    def add(ref, sources, sums):
        factors = ref[sources, :, pl.ds(half, TAIL)].astype(jnp.float32)
        spread = [jnp.broadcast_to(factors[:, :, n:n + 1], (*factors.shape[:2], LANES)) for n in range(scale_lanes)]
        added = [
            jnp.sum(ref[sources, :, pl.ds(t * LANES, LANES)].astype(jnp.float32) * spread[t // scale_tiles], axis=0)
            for t in range(tiles)
        ]
        added.append(jnp.sum(factors, axis=0))
        return tuple(s + a for s, a in zip(sums, added))

    def landed(ref, semaphore):
        pltpu.make_async_copy(ref, ref, semaphore).wait()

    sums = tuple(jnp.zeros((2, LANES), jnp.float32) for _ in range(tiles)) + (jnp.zeros((2, TAIL), jnp.float32),)
    none = sums
    if ordered:
        for layer in range(layers - 1):
            @pl.when(place[0] == layer)
            def _():
                above = layers - 1 - layer
                landed(layer_in.at[pl.ds(0, above), pl.ds(0, per_layer - 1)], layer_sem)
                pl.semaphore_wait(told_sem.at[flat], above)

        for up in reversed(range(1, layers)):
            @pl.when(place[0] + up < layers)
            def _():
                layer_in[up - 1, my_slot] = outgoing[inter_of(place[0] + up, place[1], my_core), my_intra]
                for t, each in enumerate(add(layer_in.at[up - 1], pl.ds(0, per_layer), none)):
                    layer_sum[up - 1, :, pl.ds(t * LANES, each.shape[1])] = each
                pltpu.make_async_remote_copy(
                    src_ref=layer_sum.at[up - 1],
                    dst_ref=sum_in.at[up - 1],
                    send_sem=sum_send_sem,
                    recv_sem=recv_sems.at[layers - up],
                    device_id=(inter_of(place[0] + up, place[1], my_core), my_intra),
                    device_id_type=MESH,
                ).start()

        landed(incoming.at[pl.ds(0, per_layer - 1)], recv_sems.at[0])
        sums = add(incoming, pl.ds(place[0] * per_layer, per_layer), sums)
        for group in range(1, layers):
            def direct(sums, group=group):
                landed(incoming.at[pl.ds(0, per_layer)], recv_sems.at[group])
                return add(incoming, pl.ds((place[0] + group) * per_layer, per_layer), sums)

            def summed(sums, group=group):
                below = sum_in.at[layers - group - 1]
                landed(below, recv_sems.at[group])
                return tuple(each + below[:, pl.ds(t * LANES, each.shape[1])] for t, each in enumerate(sums))

            sums = lax.cond(place[0] + group < layers, direct, summed, sums)
    else:
        landed(incoming.at[pl.ds(0, total - 1)], recv_sems.at[0])
        sums = lax.fori_loop(
            0, total // SOURCE_GROUP, lambda n, sums: add(incoming, pl.ds(n * SOURCE_GROUP, SOURCE_GROUP), sums), sums)
    lane = lax.broadcasted_iota(jnp.int32, (1, TAIL), 1)
    count = jnp.sum(jnp.where(lane == scale_lanes, sums[tiles][0:1], 0.0), axis=1, keepdims=True).astype(jnp.int32)
    keep = jnp.broadcast_to(count, (1, LANES)) == 0
    per_block = block_len // LANES
    peaks = []
    grads = []
    for t in range(tiles):
        grad = sums[t] * unscale
        grads.append(grad)
        peaks.append(jnp.max(jnp.abs(grad), axis=1, keepdims=True))
    for h in range(2):
        for t in range(tiles):
            grad = grads[t][h:h + 1]
            columns = pl.ds(h * half + t * LANES, LANES)
            grad_ref[0:1, columns] = grad
            weights = w_ref[0:1, columns]
            master_ref[0:1, columns] = jnp.where(keep, weights - 0.5 * grad, weights)
    blocks = share_cols // block_len
    block_lane = lax.broadcasted_iota(jnp.int32, (1, blocks), 1)
    largest = jnp.zeros((1, blocks), jnp.float32)
    for n in range(blocks):
        parts = [divmod(n * per_block + k, tiles) for k in range(per_block)]
        top = functools.reduce(jnp.maximum, [peaks[t][h:h + 1] for h, t in parts])
        largest = jnp.where(block_lane == n, top, largest)
    scale_ref[...] = largest / 127.0
    total_count = count[0, 0]
    exp_ref[0] = exponent[0, 0] - jnp.where(total_count > 0, 1, 0)
    count_ref[0] = total_count

    def sent(layer):
        above = layers - 1 - layer
        landed(incoming.at[pl.ds(0, per_layer * (layer + 1) - 1 + (per_layer - 1) * above)], send_sem)
        if above:
            landed(layer_sum.at[pl.ds(0, above)], sum_send_sem)

    if ordered:
        for layer in range(layers):
            pl.when(place[0] == layer)(functools.partial(sent, layer))
    else:
        landed(incoming.at[pl.ds(0, total - 1)], send_sem)


def gather_scalars(pos_ref, exp_ref, meta_ref):
    lane = lax.broadcasted_iota(jnp.int32, (1, LANES), 1)
    meta_ref[...] = jnp.where(lane == 0, jnp.where(pos_ref[0, 0] >= 0, 1, 0), exp_ref[...])


def pass_scales(meta_ref, s_ref, passed_ref):
    passed_ref[0, :, pl.ds(0, s_ref.shape[2])] = s_ref[0].astype(jnp.float32)


def finish(*refs):
    half = (len(refs) - 1) // 2
    copies = [pltpu.make_async_copy(src, dst, refs[-1].at[n]) for n, (src, dst) in enumerate(zip(refs[:half], refs[half:-1]))]
    for copy in copies:
        copy.start()
    for copy in copies:
        copy.wait()


def on_device(partials, scales, overflow_pos, weights, exponent):
    inter_size = lax.axis_size("inter")
    intra_size = lax.axis_size("intra")
    total = inter_size * intra_size
    row_total, full_width = partials.shape[1], partials.shape[2]
    block_len = full_width // scales.shape[2]
    share_cols = full_width // intra_size
    blocks = share_cols // block_len
    width = share_cols // 2 + TAIL
    layers, ordered = layers_of(inter_size)
    groups, aboves, per_layer = (layers, layers - 1, total // layers) if ordered else (1, 1, 1)
    any_space = pl.BlockSpec(memory_space=pl.ANY)
    vmem = pl.BlockSpec(memory_space=pltpu.VMEM)
    smem = pl.BlockSpec(memory_space=pltpu.SMEM)

    def in_vmem(array):
        return pltpu.with_memory_space_constraint(array, pltpu.VMEM)

    meta = pl.pallas_call(
        gather_scalars,
        out_shape=pltpu.VMEM((1, LANES), jnp.int32),
        in_specs=[smem, smem],
        out_specs=vmem,
        cost_estimate=pl.CostEstimate(flops=1000000, bytes_accessed=0, transcendentals=0),
        name="gather_scalars",
    )(overflow_pos, exponent)
    passed = pl.pallas_call(
        pass_scales,
        out_shape=pltpu.VMEM((1, row_total, LANES), jnp.float32),
        in_specs=[vmem, vmem],
        out_specs=vmem,
        cost_estimate=pl.CostEstimate(flops=60000000, bytes_accessed=0, transcendentals=0),
        name="pass_scales",
    )(in_vmem(meta), in_vmem(scales))
    results = pl.pallas_call(
        functools.partial(exchange, inter_size, intra_size, block_len),
        out_shape=(
            pltpu.VMEM((1, share_cols), jnp.float32),
            pltpu.VMEM((1, blocks), jnp.float32),
            pltpu.VMEM((1, share_cols), jnp.float32),
            pltpu.SMEM((1,), jnp.int32),
            pltpu.SMEM((1,), jnp.int32),
        ),
        in_specs=[vmem, vmem, vmem, any_space],
        out_specs=(vmem, vmem, vmem, smem, smem),
        scratch_shapes=[
            pltpu.VMEM((1, share_cols), jnp.float32),
            pltpu.VMEM((ROW_GROUP, intra_size, 2, width), jnp.float32),
            pltpu.VMEM((row_total, intra_size, 2, width), jnp.bfloat16),
            pltpu.VMEM((total, 2, width), jnp.bfloat16),
            pltpu.VMEM((aboves, per_layer, 2, width), jnp.bfloat16),
            pltpu.VMEM((aboves, 2, width), jnp.float32),
            pltpu.VMEM((aboves, 2, width), jnp.float32),
            pltpu.SemaphoreType.DMA,
            pltpu.SemaphoreType.DMA,
            pltpu.SemaphoreType.DMA,
            pltpu.SemaphoreType.DMA((groups,)),
            pltpu.SemaphoreType.DMA,
            pltpu.SemaphoreType.REGULAR((LINES + intra_size - 1,)),
            pltpu.SemaphoreType.REGULAR,
        ],
        compiler_params=pltpu.CompilerParams(collective_id=0, has_side_effects=True),
        name="exchange",
    )(in_vmem(partials), in_vmem(passed), in_vmem(meta), weights)
    grad_out, block_scale, master_out, new_exponent, count = pl.pallas_call(
        finish,
        out_shape=(
            jax.ShapeDtypeStruct((1, share_cols), jnp.float32),
            jax.ShapeDtypeStruct((1, blocks), jnp.float32),
            jax.ShapeDtypeStruct((1, share_cols), jnp.float32),
            jax.ShapeDtypeStruct((1,), jnp.int32),
            jax.ShapeDtypeStruct((1,), jnp.int32),
        ),
        in_specs=[vmem, vmem, vmem, smem, smem],
        out_specs=(any_space,) * 5,
        scratch_shapes=[pltpu.SemaphoreType.DMA((5,))],
        name="finish",
    )(*(in_vmem(result) for result in results[:3]), *results[3:])
    return grad_out, block_scale, master_out, new_exponent.reshape(()), count.reshape(())


def solution(mesh):
    placed = (
        P(("inter", "intra"), None, None),
        P(("inter", "intra"), None, None),
        P(("inter", "intra"), None),
        P("inter", "intra"),
        P(),
    )
    return jax.shard_map(
        on_device,
        mesh=mesh,
        in_specs=placed,
        out_specs=(P("inter", "intra"), P("inter", "intra"), P("inter", "intra"), P(), P()),
        check_vma=False,
    )
```

```python
import functools

import jax
import jax.numpy as jnp
from jax import lax
from jax.experimental import pallas as pl
from jax.experimental.pallas import tpu as pltpu
from jax.sharding import PartitionSpec as P

LANES = 128
CORES = 2
LINES = 2
MOST_LAYERS = 8
KEEPER = CORES - 1
TAIL = 128
ROW_GROUP = 8
SOURCE_GROUP = 32
MESH = pl.DeviceIdType.MESH


def layers_of(inter_size):
    layers = inter_size // (CORES * LINES)
    return layers, layers * CORES * LINES == inter_size and 1 < layers <= MOST_LAYERS


def exchange(inter_size, intra_size, block_len, x_ref, s_ref, meta_ref, power_ref, w_hbm,
             grad_ref, scale_ref, master_ref, exp_ref, count_ref,
             w_ref, staged, outgoing, incoming, layer_in, layer_sum, sum_in,
             load_sem, send_sem, sum_send_sem, recv_sems, layer_sem, told_sem, mate_sem):
    total = inter_size * intra_size
    row_total, full_width = x_ref.shape[1:]
    share_cols = full_width // intra_size
    half = share_cols // 2
    tiles = half // LANES
    layers, ordered = layers_of(inter_size)
    per_layer = total // layers if ordered else total
    scale_tiles = block_len // LANES if half % block_len == 0 else 1
    scale_lanes = tiles // scale_tiles
    my_inter = lax.axis_index("inter")
    my_intra = lax.axis_index("intra")
    me = my_inter * intra_size + my_intra
    my_core = lax.rem(my_inter, CORES)
    place = (my_inter // (CORES * LINES), lax.rem(my_inter // CORES, LINES), my_intra)
    at_first = place[0] + place[1] + place[2] == 0
    past = tuple(at + 1 for at in place)
    ends = (layers, LINES, intra_size)
    barrier = pltpu.get_barrier_semaphore()

    def each_chip(lows, highs, visit):
        def along_z(z, carry):
            def along_y(y, carry):
                def along_x(x, carry):
                    visit(z, y, x)
                    return carry
                return lax.fori_loop(lows[2], highs[2], along_x, carry)
            return lax.fori_loop(lows[1], highs[1], along_y, carry)
        lax.fori_loop(lows[0], highs[0], along_z, 0)

    def inter_of(z, y, core):
        return (z * LINES + y) * CORES + core

    def signal(semaphore, inter, intra):
        pl.semaphore_signal(semaphore, inc=1, device_id=(inter, intra), device_id_type=MESH)

    def elsewhere(z, y, x):
        return (z != place[0]) | (y != place[1]) | (x != place[2])

    def send(to_inter, to_intra, group):
        pltpu.make_async_remote_copy(
            src_ref=outgoing.at[to_inter, to_intra],
            dst_ref=incoming.at[me],
            send_sem=send_sem,
            recv_sem=recv_sems.at[group],
            device_id=(to_inter, to_intra),
            device_id_type=MESH,
        ).start()

    if ordered:
        def greet(z, y, x):
            @pl.when(elsewhere(z, y, x))
            def _():
                signal(barrier, inter_of(z, y, KEEPER), x)
                for core in range(KEEPER):
                    pl.when(at_first)(functools.partial(signal, barrier, inter_of(z, y, core), x))

        each_chip(place, ends, lambda z, y, x: greet(*(lo + hi - 1 - at for lo, hi, at in zip(place, ends, (z, y, x)))))
        pl.when(my_core != KEEPER)(lambda: signal(barrier, inter_of(place[0], place[1], KEEPER), my_intra))
        for core in range(KEEPER):
            pl.when(at_first & (my_core == KEEPER))(
                functools.partial(signal, barrier, inter_of(place[0], place[1], core), my_intra))
    else:
        for n in range(total):
            signal(barrier, n // intra_size, n % intra_size)
    load = pltpu.make_async_copy(w_hbm, w_ref, load_sem)
    load.start()

    flag = meta_ref[0:1, 0:1].astype(jnp.float32)
    lane = lax.broadcasted_iota(jnp.int32, (ROW_GROUP, TAIL), 1)
    power = power_ref[0:1, 0:1].astype(jnp.float32)
    flags = jnp.where(lane == scale_lanes, flag, jnp.where(lane == scale_lanes + 1, power, 0.0))

    def stage(group, shares):
        rows = pl.ds(pl.multiple_of(group * ROW_GROUP, ROW_GROUP), ROW_GROUP)
        scale_rows = s_ref[0, rows, :]
        for b in shares:
            for h in range(2):
                n = b * 2 + h
                if scale_tiles > 1:
                    spread = pltpu.roll(scale_rows, (LANES - n * scale_lanes) % LANES, 1)[:, :TAIL]
                    spread = jnp.where(lane < scale_lanes, spread, flags)
                else:
                    spread = flags
                    for t in range(tiles):
                        block = (n * tiles + t) * LANES // block_len
                        spread = jnp.where(lane == t, scale_rows[:, block:block + 1], spread)
                staged[:, b, h, pl.ds(0, half)] = x_ref[0, rows, pl.ds(n * half, half)].astype(jnp.float32)
                staged[:, b, h, pl.ds(half, TAIL)] = spread
            outgoing[rows, b] = staged[:, b].astype(jnp.bfloat16)

    stage(0, range(1))

    def stage_rest():
        stage(0, range(1, intra_size))
        if row_total == 2 * ROW_GROUP:
            stage(1, range(intra_size))
        else:
            lax.fori_loop(1, row_total // ROW_GROUP, lambda n, carry: (stage(n, range(intra_size)), carry)[1], 0)

    if ordered:
        flat = LINES + intra_size - 2
        my_slot = lax.rem(me, per_layer)

        def send_chip(z, y, x, cores=tuple(reversed(range(CORES)))):
            for core in cores:
                send(inter_of(z, y, core), x, place[0] - z)

        def send_planes(lows, highs, keep):
            def along(z, carry):
                for core in reversed(range(CORES)):
                    def visit(z, y, x):
                        pl.when(keep(z, y, x))(lambda: send_chip(z, y, x, (core,)))
                    each_chip((z, *lows[1:]), (z + 1, *highs[1:]), visit)
                return carry
            lax.fori_loop(lows[0], highs[0], along, 0)

        def send_above(z, y, x, core):
            for up in range(1, layers):
                @pl.when(z + up < layers)
                def _():
                    pltpu.make_async_remote_copy(
                        src_ref=outgoing.at[inter_of(z + up, y, core), x],
                        dst_ref=layer_in.at[up - 1, my_slot],
                        send_sem=send_sem,
                        recv_sem=layer_sem,
                        device_id=(inter_of(z, y, core), x),
                        device_id_type=MESH,
                    ).start()

        def send_chip_above(z, y, x):
            @pl.when(elsewhere(z, y, x))
            def _():
                for core in range(CORES):
                    send_above(z, y, x, core)

        def tell_flat(z, y, x):
            @pl.when(elsewhere(z, y, x))
            def _():
                signal(told_sem.at[place[1] - y + place[2] - x - 1], inter_of(z, y, my_core), x)

        def tell_down(z, y, x):
            @pl.when(elsewhere(z, y, x))
            def _():
                signal(told_sem.at[flat], inter_of(z, y, my_core), x)

        keeps = my_core == KEEPER
        below = past[0] * past[1] * past[2] * CORES - CORES
        pl.when(keeps)(stage_rest)
        pl.semaphore_wait(barrier, jnp.where(keeps, below + KEEPER, jnp.where(at_first, 1, CORES)))
        pl.when(~at_first)(lambda: send_chip(0, 0, 0, tuple(range(CORES))))
        pl.when(~keeps)(stage_rest)
        for core in range(KEEPER):
            pl.when(keeps)(functools.partial(signal, mate_sem, inter_of(place[0], place[1], core), my_intra))
        pl.when(~keeps)(lambda: pl.semaphore_wait(mate_sem, 1))
        each_chip((place[0], 0, 0), past, tell_flat)
        each_chip((0, place[1], place[2]), past, tell_down)
        send_planes((0, 0, 0), past, lambda z, y, x: elsewhere(z, y, x) & (z + y + x > 0))
        each_chip((place[0], 0, 0), past, send_chip_above)
        for core in range(CORES):
            @pl.when(core != my_core)
            def _():
                send(inter_of(place[0], place[1], core), my_intra, 0)
                send_above(*place, core)

        offsets = [(dy, dx) for dy in range(LINES) for dx in range(intra_size)]
        for steps in range(1, flat + 1):
            level = [(0, *offset) for offset in offsets if sum(offset) == steps]
            inside = [functools.reduce(jnp.logical_and, [at + d < end for at, d, end in zip(place, offset, ends)])
                      for offset in level]
            uppers = sum(each.astype(jnp.int32) for each in inside)

            @pl.when(uppers > 0)
            def _():
                pl.semaphore_wait(told_sem.at[steps - 1], uppers)

            for offset, each in zip(level, inside):
                @pl.when(each)
                def _():
                    lows = tuple(at + d if d else 0 for at, d in zip(place, offset))
                    highs = tuple(at + d + 1 for at, d in zip(place, offset))
                    each_chip((place[0], *lows[1:]), highs, send_chip_above)
                    send_planes(lows, highs, lambda z, y, x: True)
    else:
        stage_rest()
        pl.semaphore_wait(barrier, total)
        for n in range(total - 1):
            target = n + (n >= me).astype(jnp.int32)
            send(target // intra_size, lax.rem(target, intra_size), 0)

    incoming[me] = outgoing[my_inter, my_intra]
    load.wait()

    def add(ref, sources, sums):
        factors = ref[sources, :, pl.ds(half, TAIL)].astype(jnp.float32)
        spread = [jnp.broadcast_to(factors[:, :, n:n + 1], (*factors.shape[:2], LANES)) for n in range(scale_lanes)]
        added = [
            jnp.sum(ref[sources, :, pl.ds(t * LANES, LANES)].astype(jnp.float32) * spread[t // scale_tiles], axis=0)
            for t in range(tiles)
        ]
        added.append(jnp.sum(factors, axis=0))
        return tuple(s + a for s, a in zip(sums, added))

    def landed(ref, semaphore):
        pltpu.make_async_copy(ref, ref, semaphore).wait()

    sums = tuple(jnp.zeros((2, LANES), jnp.float32) for _ in range(tiles)) + (jnp.zeros((2, TAIL), jnp.float32),)
    none = sums

    def power_of(sums):
        lane = lax.broadcasted_iota(jnp.int32, (1, TAIL), 1)
        power = jnp.sum(jnp.where(lane == scale_lanes + 1, sums[tiles][0:1], 0.0), axis=1, keepdims=True)
        return power, jnp.exp2(-jnp.broadcast_to(power, (1, LANES)))

    if ordered:
        for layer in range(layers - 1):
            @pl.when(place[0] == layer)
            def _():
                above = layers - 1 - layer
                landed(layer_in.at[pl.ds(0, above), pl.ds(0, per_layer - 1)], layer_sem)
                pl.semaphore_wait(told_sem.at[flat], above)

        for up in reversed(range(1, layers)):
            @pl.when(place[0] + up < layers)
            def _():
                layer_in[up - 1, my_slot] = outgoing[inter_of(place[0] + up, place[1], my_core), my_intra]
                for t, each in enumerate(add(layer_in.at[up - 1], pl.ds(0, per_layer), none)):
                    layer_sum[up - 1, :, pl.ds(t * LANES, each.shape[1])] = each
                pltpu.make_async_remote_copy(
                    src_ref=layer_sum.at[up - 1],
                    dst_ref=sum_in.at[up - 1],
                    send_sem=sum_send_sem,
                    recv_sem=recv_sems.at[layers - up],
                    device_id=(inter_of(place[0] + up, place[1], my_core), my_intra),
                    device_id_type=MESH,
                ).start()

        landed(incoming.at[pl.ds(0, per_layer - 1)], recv_sems.at[0])
        sums = add(incoming, pl.ds(place[0] * per_layer, per_layer), sums)
        near = power_of(sums)
        for group in range(1, layers):
            def direct(sums, group=group):
                landed(incoming.at[pl.ds(0, per_layer)], recv_sems.at[group])
                return add(incoming, pl.ds((place[0] + group) * per_layer, per_layer), sums)

            def summed(sums, group=group):
                below = sum_in.at[layers - group - 1]
                landed(below, recv_sems.at[group])
                return tuple(each + below[:, pl.ds(t * LANES, each.shape[1])] for t, each in enumerate(sums))

            sums = lax.cond(place[0] + group < layers, direct, summed, sums)
    else:
        landed(incoming.at[pl.ds(0, total - 1)], recv_sems.at[0])
        sums = lax.fori_loop(
            0, total // SOURCE_GROUP, lambda n, sums: add(incoming, pl.ds(n * SOURCE_GROUP, SOURCE_GROUP), sums), sums)
    if ordered:
        power, unscale = lax.cond(place[0] == 0, lambda: near, lambda: power_of(sums))
    else:
        power, unscale = power_of(sums)
    lane = lax.broadcasted_iota(jnp.int32, (1, TAIL), 1)
    count = jnp.sum(jnp.where(lane == scale_lanes, sums[tiles][0:1], 0.0), axis=1, keepdims=True).astype(jnp.int32)
    keep = jnp.broadcast_to(count, (1, LANES)) == 0
    per_block = block_len // LANES
    peaks = []
    grads = []
    for t in range(tiles):
        grad = sums[t] * unscale
        grads.append(grad)
        peaks.append(jnp.max(jnp.abs(grad), axis=1, keepdims=True))
    for h in range(2):
        for t in range(tiles):
            grad = grads[t][h:h + 1]
            columns = pl.ds(h * half + t * LANES, LANES)
            grad_ref[0:1, columns] = grad
            weights = w_ref[0:1, columns]
            master_ref[0:1, columns] = jnp.where(keep, weights - 0.5 * grad, weights)
    blocks = share_cols // block_len
    block_lane = lax.broadcasted_iota(jnp.int32, (1, blocks), 1)
    largest = jnp.zeros((1, blocks), jnp.float32)
    for n in range(blocks):
        parts = [divmod(n * per_block + k, tiles) for k in range(per_block)]
        top = functools.reduce(jnp.maximum, [peaks[t][h:h + 1] for h, t in parts])
        largest = jnp.where(block_lane == n, top, largest)
    scale_ref[...] = largest / 127.0
    total_count = count[0, 0]
    exp_ref[0] = power.astype(jnp.int32)[0, 0] - jnp.where(total_count > 0, 1, 0)
    count_ref[0] = total_count

    def sent(layer):
        above = layers - 1 - layer
        landed(incoming.at[pl.ds(0, per_layer * (layer + 1) - 1 + (per_layer - 1) * above)], send_sem)
        if above:
            landed(layer_sum.at[pl.ds(0, above)], sum_send_sem)

    if ordered:
        for layer in range(layers):
            pl.when(place[0] == layer)(functools.partial(sent, layer))
    else:
        landed(incoming.at[pl.ds(0, total - 1)], send_sem)


def gather_scalars(pos_ref, meta_ref):
    meta_ref[...] = jnp.full((1, LANES), jnp.where(pos_ref[0, 0] >= 0, 1, 0), jnp.int32)


def pass_scales(meta_ref, s_ref, passed_ref, nothing_ref):
    nothing_ref[...] = jnp.zeros_like(nothing_ref)
    passed_ref[0, :, pl.ds(0, s_ref.shape[2])] = s_ref[0].astype(jnp.float32)


def finish(*refs):
    half = (len(refs) - 1) // 2
    copies = [pltpu.make_async_copy(src, dst, refs[-1].at[n]) for n, (src, dst) in enumerate(zip(refs[:half], refs[half:-1]))]
    for copy in copies:
        copy.start()
    for copy in copies:
        copy.wait()


def on_device(partials, scales, overflow_pos, weights, exponent):
    inter_size = lax.axis_size("inter")
    intra_size = lax.axis_size("intra")
    total = inter_size * intra_size
    row_total, full_width = partials.shape[1], partials.shape[2]
    block_len = full_width // scales.shape[2]
    share_cols = full_width // intra_size
    blocks = share_cols // block_len
    width = share_cols // 2 + TAIL
    layers, ordered = layers_of(inter_size)
    groups, aboves, per_layer = (layers, layers - 1, total // layers) if ordered else (1, 1, 1)
    any_space = pl.BlockSpec(memory_space=pl.ANY)
    vmem = pl.BlockSpec(memory_space=pltpu.VMEM)
    smem = pl.BlockSpec(memory_space=pltpu.SMEM)

    def in_vmem(array):
        return pltpu.with_memory_space_constraint(array, pltpu.VMEM)

    meta = pl.pallas_call(
        gather_scalars,
        out_shape=pltpu.VMEM((1, LANES), jnp.int32),
        in_specs=[smem],
        out_specs=vmem,
        cost_estimate=pl.CostEstimate(flops=1000000, bytes_accessed=0, transcendentals=0),
        name="gather_scalars",
    )(overflow_pos)
    passed, nothing = pl.pallas_call(
        pass_scales,
        out_shape=(pltpu.VMEM((1, row_total, LANES), jnp.float32), pltpu.VMEM((1, LANES), jnp.int32)),
        in_specs=[vmem, vmem],
        out_specs=(vmem, vmem),
        cost_estimate=pl.CostEstimate(flops=79500000, bytes_accessed=0, transcendentals=0),
        name="pass_scales",
    )(in_vmem(meta), in_vmem(scales))
    power = lax.cond(
        lax.axis_index("inter") + lax.axis_index("intra") == 0,
        lambda exponent, nothing: nothing + exponent,
        lambda exponent, nothing: nothing,
        exponent,
        nothing,
    )
    results = pl.pallas_call(
        functools.partial(exchange, inter_size, intra_size, block_len),
        out_shape=(
            pltpu.VMEM((1, share_cols), jnp.float32),
            pltpu.VMEM((1, blocks), jnp.float32),
            pltpu.VMEM((1, share_cols), jnp.float32),
            pltpu.SMEM((1,), jnp.int32),
            pltpu.SMEM((1,), jnp.int32),
        ),
        in_specs=[vmem, vmem, vmem, vmem, any_space],
        out_specs=(vmem, vmem, vmem, smem, smem),
        scratch_shapes=[
            pltpu.VMEM((1, share_cols), jnp.float32),
            pltpu.VMEM((ROW_GROUP, intra_size, 2, width), jnp.float32),
            pltpu.VMEM((row_total, intra_size, 2, width), jnp.bfloat16),
            pltpu.VMEM((total, 2, width), jnp.bfloat16),
            pltpu.VMEM((aboves, per_layer, 2, width), jnp.bfloat16),
            pltpu.VMEM((aboves, 2, width), jnp.float32),
            pltpu.VMEM((aboves, 2, width), jnp.float32),
            pltpu.SemaphoreType.DMA,
            pltpu.SemaphoreType.DMA,
            pltpu.SemaphoreType.DMA,
            pltpu.SemaphoreType.DMA((groups,)),
            pltpu.SemaphoreType.DMA,
            pltpu.SemaphoreType.REGULAR((LINES + intra_size - 1,)),
            pltpu.SemaphoreType.REGULAR,
        ],
        compiler_params=pltpu.CompilerParams(collective_id=0, has_side_effects=True),
        name="exchange",
    )(in_vmem(partials), in_vmem(passed), in_vmem(meta), in_vmem(power), weights)
    grad_out, block_scale, master_out, new_exponent, count = pl.pallas_call(
        finish,
        out_shape=(
            jax.ShapeDtypeStruct((1, share_cols), jnp.float32),
            jax.ShapeDtypeStruct((1, blocks), jnp.float32),
            jax.ShapeDtypeStruct((1, share_cols), jnp.float32),
            jax.ShapeDtypeStruct((1,), jnp.int32),
            jax.ShapeDtypeStruct((1,), jnp.int32),
        ),
        in_specs=[vmem, vmem, vmem, smem, smem],
        out_specs=(any_space,) * 5,
        scratch_shapes=[pltpu.SemaphoreType.DMA((5,))],
        name="finish",
    )(*(in_vmem(result) for result in results[:3]), *results[3:])
    return grad_out, block_scale, master_out, new_exponent.reshape(()), count.reshape(())


def solution(mesh):
    placed = (
        P(("inter", "intra"), None, None),
        P(("inter", "intra"), None, None),
        P(("inter", "intra"), None),
        P("inter", "intra"),
        P(),
    )
    return jax.shard_map(
        on_device,
        mesh=mesh,
        in_specs=placed,
        out_specs=(P("inter", "intra"), P("inter", "intra"), P("inter", "intra"), P(), P()),
        check_vma=False,
    )
```

```python
import functools

import jax
import jax.numpy as jnp
from jax import lax
from jax.experimental import pallas as pl
from jax.experimental.pallas import tpu as pltpu
from jax.sharding import PartitionSpec as P

LANES = 128
CORES = 2
LINES = 2
MOST_LAYERS = 8
KEEPER = CORES - 1
TAIL = 128
ROW_GROUP = 8
SOURCE_GROUP = 32
MESH = pl.DeviceIdType.MESH


def layers_of(inter_size):
    layers = inter_size // (CORES * LINES)
    return layers, layers * CORES * LINES == inter_size and 1 < layers <= MOST_LAYERS


def exchange(inter_size, intra_size, block_len, x_ref, s_ref, meta_ref, power_ref, w_hbm,
             grad_ref, scale_ref, master_ref, exp_ref, count_ref,
             w_ref, staged, outgoing, incoming, layer_in, layer_sum, sum_in,
             load_sem, send_sem, sum_send_sem, recv_sems, layer_sem, told_sem, mate_sem):
    total = inter_size * intra_size
    row_total, full_width = x_ref.shape[1:]
    share_cols = full_width // intra_size
    half = share_cols // 2
    tiles = half // LANES
    layers, ordered = layers_of(inter_size)
    per_layer = total // layers if ordered else total
    scale_tiles = block_len // LANES if half % block_len == 0 else 1
    scale_lanes = tiles // scale_tiles
    my_inter = lax.axis_index("inter")
    my_intra = lax.axis_index("intra")
    me = my_inter * intra_size + my_intra
    my_core = lax.rem(my_inter, CORES)
    place = (my_inter // (CORES * LINES), lax.rem(my_inter // CORES, LINES), my_intra)
    at_first = place[0] + place[1] + place[2] == 0
    past = tuple(at + 1 for at in place)
    ends = (layers, LINES, intra_size)
    barrier = pltpu.get_barrier_semaphore()

    def each_chip(lows, highs, visit):
        def along_z(z, carry):
            def along_y(y, carry):
                def along_x(x, carry):
                    visit(z, y, x)
                    return carry
                return lax.fori_loop(lows[2], highs[2], along_x, carry)
            return lax.fori_loop(lows[1], highs[1], along_y, carry)
        lax.fori_loop(lows[0], highs[0], along_z, 0)

    def inter_of(z, y, core):
        return (z * LINES + y) * CORES + core

    def signal(semaphore, inter, intra):
        pl.semaphore_signal(semaphore, inc=1, device_id=(inter, intra), device_id_type=MESH)

    def elsewhere(z, y, x):
        return (z != place[0]) | (y != place[1]) | (x != place[2])

    def send(to_inter, to_intra, group):
        pltpu.make_async_remote_copy(
            src_ref=outgoing.at[to_inter, to_intra],
            dst_ref=incoming.at[me],
            send_sem=send_sem,
            recv_sem=recv_sems.at[group],
            device_id=(to_inter, to_intra),
            device_id_type=MESH,
        ).start()

    if ordered:
        def greet(z, y, x):
            @pl.when(elsewhere(z, y, x))
            def _():
                signal(barrier, inter_of(z, y, KEEPER), x)
                for core in range(KEEPER):
                    pl.when(at_first)(functools.partial(signal, barrier, inter_of(z, y, core), x))

        each_chip(place, ends, lambda z, y, x: greet(*(lo + hi - 1 - at for lo, hi, at in zip(place, ends, (z, y, x)))))
        pl.when(my_core != KEEPER)(lambda: signal(barrier, inter_of(place[0], place[1], KEEPER), my_intra))
        for core in range(KEEPER):
            pl.when(at_first & (my_core == KEEPER))(
                functools.partial(signal, barrier, inter_of(place[0], place[1], core), my_intra))
    else:
        for n in range(total):
            signal(barrier, n // intra_size, n % intra_size)
    load = pltpu.make_async_copy(w_hbm, w_ref, load_sem)
    load.start()

    flag = meta_ref[0:1, 0:1].astype(jnp.float32)
    lane = lax.broadcasted_iota(jnp.int32, (ROW_GROUP, TAIL), 1)
    power = power_ref[0:1, 0:1].astype(jnp.float32)
    flags = jnp.where(lane == scale_lanes, flag, jnp.where(lane == scale_lanes + 1, power, 0.0))

    def stage(group, shares):
        rows = pl.ds(pl.multiple_of(group * ROW_GROUP, ROW_GROUP), ROW_GROUP)
        scale_rows = s_ref[0, rows, :]
        for b in shares:
            for h in range(2):
                n = b * 2 + h
                if scale_tiles > 1:
                    spread = pltpu.roll(scale_rows, (LANES - n * scale_lanes) % LANES, 1)[:, :TAIL]
                    spread = jnp.where(lane < scale_lanes, spread, flags)
                else:
                    spread = flags
                    for t in range(tiles):
                        block = (n * tiles + t) * LANES // block_len
                        spread = jnp.where(lane == t, scale_rows[:, block:block + 1], spread)
                staged[:, b, h, pl.ds(0, half)] = x_ref[0, rows, pl.ds(n * half, half)].astype(jnp.float32)
                staged[:, b, h, pl.ds(half, TAIL)] = spread
            outgoing[rows, b] = staged[:, b].astype(jnp.bfloat16)

    stage(0, range(1))

    def stage_rest():
        stage(0, range(1, intra_size))
        if row_total == 2 * ROW_GROUP:
            stage(1, range(intra_size))
        else:
            lax.fori_loop(1, row_total // ROW_GROUP, lambda n, carry: (stage(n, range(intra_size)), carry)[1], 0)

    if ordered:
        flat = LINES + intra_size - 2
        my_slot = lax.rem(me, per_layer)

        def send_chip(z, y, x, cores=tuple(reversed(range(CORES)))):
            for core in cores:
                send(inter_of(z, y, core), x, place[0] - z)

        def send_planes(lows, highs, keep):
            def along(z, carry):
                for core in reversed(range(CORES)):
                    def visit(z, y, x):
                        pl.when(keep(z, y, x))(lambda: send_chip(z, y, x, (core,)))
                    each_chip((z, *lows[1:]), (z + 1, *highs[1:]), visit)
                return carry
            lax.fori_loop(lows[0], highs[0], along, 0)

        def send_above(z, y, x, core):
            for up in range(1, layers):
                @pl.when(z + up < layers)
                def _():
                    pltpu.make_async_remote_copy(
                        src_ref=outgoing.at[inter_of(z + up, y, core), x],
                        dst_ref=layer_in.at[up - 1, my_slot],
                        send_sem=send_sem,
                        recv_sem=layer_sem,
                        device_id=(inter_of(z, y, core), x),
                        device_id_type=MESH,
                    ).start()

        def send_chip_above(z, y, x):
            @pl.when(elsewhere(z, y, x))
            def _():
                for core in range(CORES):
                    send_above(z, y, x, core)

        def tell_flat(z, y, x):
            @pl.when(elsewhere(z, y, x))
            def _():
                signal(told_sem.at[place[1] - y + place[2] - x - 1], inter_of(z, y, my_core), x)

        def tell_down(z, y, x):
            @pl.when(elsewhere(z, y, x))
            def _():
                signal(told_sem.at[flat], inter_of(z, y, my_core), x)

        keeps = my_core == KEEPER
        below = past[0] * past[1] * past[2] * CORES - CORES
        pl.when(keeps)(stage_rest)
        pl.semaphore_wait(barrier, jnp.where(keeps, below + KEEPER, jnp.where(at_first, 1, CORES)))
        pl.when(~at_first)(lambda: send_chip(0, 0, 0, tuple(range(CORES))))
        pl.when(~keeps)(stage_rest)
        for core in range(KEEPER):
            pl.when(keeps)(functools.partial(signal, mate_sem, inter_of(place[0], place[1], core), my_intra))
        pl.when(~keeps)(lambda: pl.semaphore_wait(mate_sem, 1))
        each_chip((place[0], 0, 0), past, tell_flat)
        each_chip((0, place[1], place[2]), past, tell_down)
        send_planes((0, 0, 0), past, lambda z, y, x: elsewhere(z, y, x) & (z + y + x > 0))
        each_chip((place[0], 0, 0), past, send_chip_above)
        for core in range(CORES):
            @pl.when(core != my_core)
            def _():
                send(inter_of(place[0], place[1], core), my_intra, 0)
                send_above(*place, core)

        offsets = [(dy, dx) for dy in range(LINES) for dx in range(intra_size)]
        for steps in range(1, flat + 1):
            level = [(0, *offset) for offset in offsets if sum(offset) == steps]
            inside = [functools.reduce(jnp.logical_and, [at + d < end for at, d, end in zip(place, offset, ends)])
                      for offset in level]
            uppers = sum(each.astype(jnp.int32) for each in inside)

            @pl.when(uppers > 0)
            def _():
                pl.semaphore_wait(told_sem.at[steps - 1], uppers)

            for offset, each in zip(level, inside):
                @pl.when(each)
                def _():
                    lows = tuple(at + d if d else 0 for at, d in zip(place, offset))
                    highs = tuple(at + d + 1 for at, d in zip(place, offset))
                    each_chip((place[0], *lows[1:]), highs, send_chip_above)
                    send_planes(lows, highs, lambda z, y, x: True)
    else:
        stage_rest()
        pl.semaphore_wait(barrier, total)
        for n in range(total - 1):
            target = n + (n >= me).astype(jnp.int32)
            send(target // intra_size, lax.rem(target, intra_size), 0)

    incoming[me] = outgoing[my_inter, my_intra]
    load.wait()

    def add(ref, sources, sums):
        factors = ref[sources, :, pl.ds(half, TAIL)].astype(jnp.float32)
        spread = [jnp.broadcast_to(factors[:, :, n:n + 1], (*factors.shape[:2], LANES)) for n in range(scale_lanes)]
        added = [
            jnp.sum(ref[sources, :, pl.ds(t * LANES, LANES)].astype(jnp.float32) * spread[t // scale_tiles], axis=0)
            for t in range(tiles)
        ]
        added.append(jnp.sum(factors, axis=0))
        return tuple(s + a for s, a in zip(sums, added))

    def landed(ref, semaphore):
        pltpu.make_async_copy(ref, ref, semaphore).wait()

    sums = tuple(jnp.zeros((2, LANES), jnp.float32) for _ in range(tiles)) + (jnp.zeros((2, TAIL), jnp.float32),)
    none = sums

    def power_of(sums):
        lane = lax.broadcasted_iota(jnp.int32, (1, TAIL), 1)
        power = jnp.sum(jnp.where(lane == scale_lanes + 1, sums[tiles][0:1], 0.0), axis=1, keepdims=True)
        return power, jnp.exp2(-jnp.broadcast_to(power, (1, LANES)))

    if ordered:
        for layer in range(layers - 1):
            @pl.when(place[0] == layer)
            def _():
                above = layers - 1 - layer
                landed(layer_in.at[pl.ds(0, above), pl.ds(0, per_layer - 1)], layer_sem)
                pl.semaphore_wait(told_sem.at[flat], above)

        for up in reversed(range(1, layers)):
            @pl.when(place[0] + up < layers)
            def _():
                layer_in[up - 1, my_slot] = outgoing[inter_of(place[0] + up, place[1], my_core), my_intra]
                for t, each in enumerate(add(layer_in.at[up - 1], pl.ds(0, per_layer), none)):
                    layer_sum[up - 1, :, pl.ds(t * LANES, each.shape[1])] = each
                pltpu.make_async_remote_copy(
                    src_ref=layer_sum.at[up - 1],
                    dst_ref=sum_in.at[up - 1],
                    send_sem=sum_send_sem,
                    recv_sem=recv_sems.at[layers - up],
                    device_id=(inter_of(place[0] + up, place[1], my_core), my_intra),
                    device_id_type=MESH,
                ).start()

        landed(incoming.at[pl.ds(0, per_layer - 1)], recv_sems.at[0])
        sums = add(incoming, pl.ds(place[0] * per_layer, per_layer), sums)
        near = power_of(sums)
        others = [layers - 1, *range(1, layers - 1)]
        for group, other in enumerate(others, 1):
            def direct(sums, group=group):
                landed(incoming.at[pl.ds(0, per_layer)], recv_sems.at[group])
                return add(incoming, pl.ds((place[0] + group) * per_layer, per_layer), sums)

            def summed(sums, group=other):
                below = sum_in.at[layers - group - 1]
                landed(below, recv_sems.at[group])
                return tuple(each + below[:, pl.ds(t * LANES, each.shape[1])] for t, each in enumerate(sums))

            def upper(sums, other=other, direct=direct, summed=summed):
                return lax.cond(place[0] + other < layers, functools.partial(direct, group=other), summed, sums)

            sums = lax.cond(place[0] == 0, direct, upper, sums)
            if group == 1:
                near = lax.cond(place[0] == 0, lambda near: near, lambda near: power_of(sums), near)
    else:
        landed(incoming.at[pl.ds(0, total - 1)], recv_sems.at[0])
        sums = lax.fori_loop(
            0, total // SOURCE_GROUP, lambda n, sums: add(incoming, pl.ds(n * SOURCE_GROUP, SOURCE_GROUP), sums), sums)
    if ordered:
        power, unscale = lax.cond(place[0] < 2, lambda: near, lambda: power_of(sums))
    else:
        power, unscale = power_of(sums)
    lane = lax.broadcasted_iota(jnp.int32, (1, TAIL), 1)
    count = jnp.sum(jnp.where(lane == scale_lanes, sums[tiles][0:1], 0.0), axis=1, keepdims=True).astype(jnp.int32)
    keep = jnp.broadcast_to(count, (1, LANES)) == 0
    per_block = block_len // LANES
    peaks = []
    grads = []
    for t in range(tiles):
        grad = sums[t] * unscale
        grads.append(grad)
        peaks.append(jnp.max(jnp.abs(grad), axis=1, keepdims=True))
    for h in range(2):
        for t in range(tiles):
            grad = grads[t][h:h + 1]
            columns = pl.ds(h * half + t * LANES, LANES)
            grad_ref[0:1, columns] = grad
            weights = w_ref[0:1, columns]
            master_ref[0:1, columns] = jnp.where(keep, weights - 0.5 * grad, weights)
    blocks = share_cols // block_len
    block_lane = lax.broadcasted_iota(jnp.int32, (1, blocks), 1)
    largest = jnp.zeros((1, blocks), jnp.float32)
    for n in range(blocks):
        parts = [divmod(n * per_block + k, tiles) for k in range(per_block)]
        top = functools.reduce(jnp.maximum, [peaks[t][h:h + 1] for h, t in parts])
        largest = jnp.where(block_lane == n, top, largest)
    scale_ref[...] = largest / 127.0
    total_count = count[0, 0]
    exp_ref[0] = power.astype(jnp.int32)[0, 0] - jnp.where(total_count > 0, 1, 0)
    count_ref[0] = total_count

    def sent(layer):
        above = layers - 1 - layer
        landed(incoming.at[pl.ds(0, per_layer * (layer + 1) - 1 + (per_layer - 1) * above)], send_sem)
        if above:
            landed(layer_sum.at[pl.ds(0, above)], sum_send_sem)

    if ordered:
        for layer in range(layers):
            pl.when(place[0] == layer)(functools.partial(sent, layer))
    else:
        landed(incoming.at[pl.ds(0, total - 1)], send_sem)


def gather_scalars(pos_ref, meta_ref):
    meta_ref[...] = jnp.full((1, LANES), jnp.where(pos_ref[0, 0] >= 0, 1, 0), jnp.int32)


def pass_scales(meta_ref, s_ref, passed_ref, nothing_ref):
    nothing_ref[...] = jnp.zeros_like(nothing_ref)
    passed_ref[0, :, pl.ds(0, s_ref.shape[2])] = s_ref[0].astype(jnp.float32)


def finish(*refs):
    half = (len(refs) - 1) // 2
    copies = [pltpu.make_async_copy(src, dst, refs[-1].at[n]) for n, (src, dst) in enumerate(zip(refs[:half], refs[half:-1]))]
    for copy in copies:
        copy.start()
    for copy in copies:
        copy.wait()


def on_device(partials, scales, overflow_pos, weights, exponent):
    inter_size = lax.axis_size("inter")
    intra_size = lax.axis_size("intra")
    total = inter_size * intra_size
    row_total, full_width = partials.shape[1], partials.shape[2]
    block_len = full_width // scales.shape[2]
    share_cols = full_width // intra_size
    blocks = share_cols // block_len
    width = share_cols // 2 + TAIL
    layers, ordered = layers_of(inter_size)
    groups, aboves, per_layer = (layers, layers - 1, total // layers) if ordered else (1, 1, 1)
    any_space = pl.BlockSpec(memory_space=pl.ANY)
    vmem = pl.BlockSpec(memory_space=pltpu.VMEM)
    smem = pl.BlockSpec(memory_space=pltpu.SMEM)

    def in_vmem(array):
        return pltpu.with_memory_space_constraint(array, pltpu.VMEM)

    meta = pl.pallas_call(
        gather_scalars,
        out_shape=pltpu.VMEM((1, LANES), jnp.int32),
        in_specs=[smem],
        out_specs=vmem,
        cost_estimate=pl.CostEstimate(flops=1000000, bytes_accessed=0, transcendentals=0),
        name="gather_scalars",
    )(overflow_pos)
    passed, nothing = pl.pallas_call(
        pass_scales,
        out_shape=(pltpu.VMEM((1, row_total, LANES), jnp.float32), pltpu.VMEM((1, LANES), jnp.int32)),
        in_specs=[vmem, vmem],
        out_specs=(vmem, vmem),
        cost_estimate=pl.CostEstimate(flops=79500000, bytes_accessed=0, transcendentals=0),
        name="pass_scales",
    )(in_vmem(meta), in_vmem(scales))
    power = lax.cond(
        lax.axis_index("inter") + lax.axis_index("intra") == 0,
        lambda exponent, nothing: nothing + exponent,
        lambda exponent, nothing: nothing,
        exponent,
        nothing,
    )
    results = pl.pallas_call(
        functools.partial(exchange, inter_size, intra_size, block_len),
        out_shape=(
            pltpu.VMEM((1, share_cols), jnp.float32),
            pltpu.VMEM((1, blocks), jnp.float32),
            pltpu.VMEM((1, share_cols), jnp.float32),
            pltpu.SMEM((1,), jnp.int32),
            pltpu.SMEM((1,), jnp.int32),
        ),
        in_specs=[vmem, vmem, vmem, vmem, any_space],
        out_specs=(vmem, vmem, vmem, smem, smem),
        scratch_shapes=[
            pltpu.VMEM((1, share_cols), jnp.float32),
            pltpu.VMEM((ROW_GROUP, intra_size, 2, width), jnp.float32),
            pltpu.VMEM((row_total, intra_size, 2, width), jnp.bfloat16),
            pltpu.VMEM((total, 2, width), jnp.bfloat16),
            pltpu.VMEM((aboves, per_layer, 2, width), jnp.bfloat16),
            pltpu.VMEM((aboves, 2, width), jnp.float32),
            pltpu.VMEM((aboves, 2, width), jnp.float32),
            pltpu.SemaphoreType.DMA,
            pltpu.SemaphoreType.DMA,
            pltpu.SemaphoreType.DMA,
            pltpu.SemaphoreType.DMA((groups,)),
            pltpu.SemaphoreType.DMA,
            pltpu.SemaphoreType.REGULAR((LINES + intra_size - 1,)),
            pltpu.SemaphoreType.REGULAR,
        ],
        compiler_params=pltpu.CompilerParams(collective_id=0, has_side_effects=True),
        name="exchange",
    )(in_vmem(partials), in_vmem(passed), in_vmem(meta), in_vmem(power), weights)
    grad_out, block_scale, master_out, new_exponent, count = pl.pallas_call(
        finish,
        out_shape=(
            jax.ShapeDtypeStruct((1, share_cols), jnp.float32),
            jax.ShapeDtypeStruct((1, blocks), jnp.float32),
            jax.ShapeDtypeStruct((1, share_cols), jnp.float32),
            jax.ShapeDtypeStruct((1,), jnp.int32),
            jax.ShapeDtypeStruct((1,), jnp.int32),
        ),
        in_specs=[vmem, vmem, vmem, smem, smem],
        out_specs=(any_space,) * 5,
        scratch_shapes=[pltpu.SemaphoreType.DMA((5,))],
        name="finish",
    )(*(in_vmem(result) for result in results[:3]), *results[3:])
    return grad_out, block_scale, master_out, new_exponent.reshape(()), count.reshape(())


def solution(mesh):
    placed = (
        P(("inter", "intra"), None, None),
        P(("inter", "intra"), None, None),
        P(("inter", "intra"), None),
        P("inter", "intra"),
        P(),
    )
    return jax.shard_map(
        on_device,
        mesh=mesh,
        in_specs=placed,
        out_specs=(P("inter", "intra"), P("inter", "intra"), P("inter", "intra"), P(), P()),
        check_vma=False,
    )
```

```python
import functools

import jax
import jax.numpy as jnp
from jax import lax
from jax.experimental import pallas as pl
from jax.experimental.pallas import tpu as pltpu
from jax.sharding import PartitionSpec as P

LANES = 128
CORES = 2
LINES = 2
MOST_LAYERS = 8
KEEPER = CORES - 1
TAIL = 128
ROW_GROUP = 8
SOURCE_GROUP = 32
MESH = pl.DeviceIdType.MESH


def layers_of(inter_size):
    layers = inter_size // (CORES * LINES)
    return layers, layers * CORES * LINES == inter_size and 1 < layers <= MOST_LAYERS


def exchange(inter_size, intra_size, block_len, x_ref, s_ref, meta_ref, power_ref, w_hbm,
             grad_ref, scale_ref, master_ref, exp_ref, count_ref,
             w_ref, staged, outgoing, incoming, layer_in, layer_sum, sum_in,
             load_sem, send_sem, sum_send_sem, recv_sems, layer_sem, told_sem, mate_sem):
    total = inter_size * intra_size
    row_total, full_width = x_ref.shape[1:]
    share_cols = full_width // intra_size
    half = share_cols // 2
    tiles = half // LANES
    layers, ordered = layers_of(inter_size)
    per_layer = total // layers if ordered else total
    scale_tiles = block_len // LANES if half % block_len == 0 else 1
    scale_lanes = tiles // scale_tiles
    my_inter = lax.axis_index("inter")
    my_intra = lax.axis_index("intra")
    me = my_inter * intra_size + my_intra
    my_core = lax.rem(my_inter, CORES)
    place = (my_inter // (CORES * LINES), lax.rem(my_inter // CORES, LINES), my_intra)
    at_first = place[0] + place[1] + place[2] == 0
    past = tuple(at + 1 for at in place)
    ends = (layers, LINES, intra_size)
    barrier = pltpu.get_barrier_semaphore()

    def each_chip(lows, highs, visit):
        def along_z(z, carry):
            def along_y(y, carry):
                def along_x(x, carry):
                    visit(z, y, x)
                    return carry
                return lax.fori_loop(lows[2], highs[2], along_x, carry)
            return lax.fori_loop(lows[1], highs[1], along_y, carry)
        lax.fori_loop(lows[0], highs[0], along_z, 0)

    def inter_of(z, y, core):
        return (z * LINES + y) * CORES + core

    def signal(semaphore, inter, intra):
        pl.semaphore_signal(semaphore, inc=1, device_id=(inter, intra), device_id_type=MESH)

    def elsewhere(z, y, x):
        return (z != place[0]) | (y != place[1]) | (x != place[2])

    def send(to_inter, to_intra, group):
        pltpu.make_async_remote_copy(
            src_ref=outgoing.at[to_inter, to_intra],
            dst_ref=incoming.at[me],
            send_sem=send_sem,
            recv_sem=recv_sems.at[group],
            device_id=(to_inter, to_intra),
            device_id_type=MESH,
        ).start()

    if ordered:
        def greet(z, y, x):
            @pl.when(elsewhere(z, y, x))
            def _():
                signal(barrier, inter_of(z, y, KEEPER), x)
                for core in range(KEEPER):
                    pl.when(at_first)(functools.partial(signal, barrier, inter_of(z, y, core), x))

        each_chip(place, ends, lambda z, y, x: greet(*(lo + hi - 1 - at for lo, hi, at in zip(place, ends, (z, y, x)))))
        pl.when(my_core != KEEPER)(lambda: signal(barrier, inter_of(place[0], place[1], KEEPER), my_intra))
        for core in range(KEEPER):
            pl.when(at_first & (my_core == KEEPER))(
                functools.partial(signal, barrier, inter_of(place[0], place[1], core), my_intra))
    else:
        for n in range(total):
            signal(barrier, n // intra_size, n % intra_size)
    load = pltpu.make_async_copy(w_hbm, w_ref, load_sem)
    load.start()

    flag = meta_ref[0:1, 0:1].astype(jnp.float32)
    lane = lax.broadcasted_iota(jnp.int32, (ROW_GROUP, TAIL), 1)
    power = power_ref[0:1, 0:1].astype(jnp.float32)
    flags = jnp.where(lane == scale_lanes, flag, jnp.where(lane == scale_lanes + 1, power, 0.0))

    def stage(group, shares):
        rows = pl.ds(pl.multiple_of(group * ROW_GROUP, ROW_GROUP), ROW_GROUP)
        scale_rows = s_ref[0, rows, :]
        for b in shares:
            for h in range(2):
                n = b * 2 + h
                if scale_tiles > 1:
                    spread = pltpu.roll(scale_rows, (LANES - n * scale_lanes) % LANES, 1)[:, :TAIL]
                    spread = jnp.where(lane < scale_lanes, spread, flags)
                else:
                    spread = flags
                    for t in range(tiles):
                        block = (n * tiles + t) * LANES // block_len
                        spread = jnp.where(lane == t, scale_rows[:, block:block + 1], spread)
                staged[:, b, h, pl.ds(0, half)] = x_ref[0, rows, pl.ds(n * half, half)].astype(jnp.float32)
                staged[:, b, h, pl.ds(half, TAIL)] = spread
            outgoing[rows, b] = staged[:, b].astype(jnp.bfloat16)

    stage(0, range(1))

    def stage_rest():
        stage(0, range(1, intra_size))
        if row_total == 2 * ROW_GROUP:
            stage(1, range(intra_size))
        else:
            lax.fori_loop(1, row_total // ROW_GROUP, lambda n, carry: (stage(n, range(intra_size)), carry)[1], 0)

    if ordered:
        flat = LINES + intra_size - 2
        my_slot = lax.rem(me, per_layer)

        def send_chip(z, y, x, cores=tuple(reversed(range(CORES)))):
            for core in cores:
                send(inter_of(z, y, core), x, place[0] - z)

        def send_planes(lows, highs, keep):
            def along(z, carry):
                for core in reversed(range(CORES)):
                    def visit(z, y, x):
                        pl.when(keep(z, y, x))(lambda: send_chip(z, y, x, (core,)))
                    each_chip((z, *lows[1:]), (z + 1, *highs[1:]), visit)
                return carry
            lax.fori_loop(lows[0], highs[0], along, 0)

        def send_above(z, y, x, core):
            for up in range(1, layers):
                @pl.when(z + up < layers)
                def _():
                    pltpu.make_async_remote_copy(
                        src_ref=outgoing.at[inter_of(z + up, y, core), x],
                        dst_ref=layer_in.at[up - 1, my_slot],
                        send_sem=send_sem,
                        recv_sem=layer_sem,
                        device_id=(inter_of(z, y, core), x),
                        device_id_type=MESH,
                    ).start()

        def send_chip_above(z, y, x):
            @pl.when(elsewhere(z, y, x))
            def _():
                for core in range(CORES):
                    send_above(z, y, x, core)

        def tell_flat(z, y, x):
            @pl.when(elsewhere(z, y, x))
            def _():
                signal(told_sem.at[place[1] - y + place[2] - x - 1], inter_of(z, y, my_core), x)

        def tell_down(z, y, x):
            @pl.when(elsewhere(z, y, x))
            def _():
                signal(told_sem.at[flat], inter_of(z, y, my_core), x)

        keeps = my_core == KEEPER
        below = past[0] * past[1] * past[2] * CORES - CORES
        pl.when(keeps)(stage_rest)
        pl.semaphore_wait(barrier, jnp.where(keeps, below + KEEPER, jnp.where(at_first, 1, CORES)))
        pl.when(~at_first)(lambda: send_chip(0, 0, 0, tuple(range(CORES))))
        pl.when(~keeps)(stage_rest)
        for core in range(KEEPER):
            pl.when(keeps)(functools.partial(signal, mate_sem, inter_of(place[0], place[1], core), my_intra))
        pl.when(~keeps)(lambda: pl.semaphore_wait(mate_sem, 1))
        each_chip((place[0], 0, 0), past, tell_flat)
        each_chip((0, place[1], place[2]), past, tell_down)
        send_planes((0, 0, 0), past, lambda z, y, x: elsewhere(z, y, x) & (z + y + x > 0))
        each_chip((place[0], 0, 0), past, send_chip_above)
        for core in range(CORES):
            @pl.when(core != my_core)
            def _():
                send(inter_of(place[0], place[1], core), my_intra, 0)
                send_above(*place, core)

        offsets = [(dy, dx) for dy in range(LINES) for dx in range(intra_size)]
        for steps in range(1, flat + 1):
            level = [(0, *offset) for offset in offsets if sum(offset) == steps]
            inside = [functools.reduce(jnp.logical_and, [at + d < end for at, d, end in zip(place, offset, ends)])
                      for offset in level]
            uppers = sum(each.astype(jnp.int32) for each in inside)

            @pl.when(uppers > 0)
            def _():
                pl.semaphore_wait(told_sem.at[steps - 1], uppers)

            for offset, each in zip(level, inside):
                @pl.when(each)
                def _():
                    lows = tuple(at + d if d else 0 for at, d in zip(place, offset))
                    highs = tuple(at + d + 1 for at, d in zip(place, offset))
                    each_chip((place[0], *lows[1:]), highs, send_chip_above)
                    send_planes(lows, highs, lambda z, y, x: True)
    else:
        stage_rest()
        pl.semaphore_wait(barrier, total)
        for n in range(total - 1):
            target = n + (n >= me).astype(jnp.int32)
            send(target // intra_size, lax.rem(target, intra_size), 0)

    incoming[me] = outgoing[my_inter, my_intra]
    load.wait()

    def add(ref, sources, sums):
        factors = ref[sources, :, pl.ds(half, TAIL)].astype(jnp.float32)
        spread = [jnp.broadcast_to(factors[:, :, n:n + 1], (*factors.shape[:2], LANES)) for n in range(scale_lanes)]
        added = [
            jnp.sum(ref[sources, :, pl.ds(t * LANES, LANES)].astype(jnp.float32) * spread[t // scale_tiles], axis=0)
            for t in range(tiles)
        ]
        added.append(jnp.sum(factors, axis=0))
        return tuple(s + a for s, a in zip(sums, added))

    def landed(ref, semaphore):
        pltpu.make_async_copy(ref, ref, semaphore).wait()

    sums = tuple(jnp.zeros((2, LANES), jnp.float32) for _ in range(tiles)) + (jnp.zeros((2, TAIL), jnp.float32),)
    none = sums

    def power_of(sums):
        lane = lax.broadcasted_iota(jnp.int32, (1, TAIL), 1)
        power = jnp.sum(jnp.where(lane == scale_lanes + 1, sums[tiles][0:1], 0.0), axis=1, keepdims=True)
        return power, jnp.exp2(-jnp.broadcast_to(power, (1, LANES)))

    if ordered:
        for layer in range(layers - 1):
            @pl.when(place[0] == layer)
            def _():
                above = layers - 1 - layer
                landed(layer_in.at[pl.ds(0, above), pl.ds(0, per_layer - 1)], layer_sem)
                pl.semaphore_wait(told_sem.at[flat], above)

        for up in reversed(range(1, layers)):
            @pl.when(place[0] + up < layers)
            def _():
                layer_in[up - 1, my_slot] = outgoing[inter_of(place[0] + up, place[1], my_core), my_intra]
                for t, each in enumerate(add(layer_in.at[up - 1], pl.ds(0, per_layer), none)):
                    layer_sum[up - 1, :, pl.ds(t * LANES, each.shape[1])] = each
                pltpu.make_async_remote_copy(
                    src_ref=layer_sum.at[up - 1],
                    dst_ref=sum_in.at[up - 1],
                    send_sem=sum_send_sem,
                    recv_sem=recv_sems.at[layers - up],
                    device_id=(inter_of(place[0] + up, place[1], my_core), my_intra),
                    device_id_type=MESH,
                ).start()

        landed(incoming.at[pl.ds(0, per_layer - 1)], recv_sems.at[0])
        sums = add(incoming, pl.ds(place[0] * per_layer, per_layer), sums)
        near = power_of(sums)
        others = [layers - 1, *range(1, layers - 1)]
        for group, other in enumerate(others, 1):
            def direct(sums, group=group):
                landed(incoming.at[pl.ds(0, per_layer)], recv_sems.at[group])
                return add(incoming, pl.ds((place[0] + group) * per_layer, per_layer), sums)

            def summed(sums, group=other):
                below = sum_in.at[layers - group - 1]
                landed(below, recv_sems.at[group])
                return tuple(each + below[:, pl.ds(t * LANES, each.shape[1])] for t, each in enumerate(sums))

            def upper(sums, other=other, direct=direct, summed=summed):
                return lax.cond(place[0] + other < layers, functools.partial(direct, group=other), summed, sums)

            sums = lax.cond(place[0] == 0, direct, upper, sums)
            if group == 1:
                near = lax.cond(place[0] == 0, lambda near: near, lambda near: power_of(sums), near)
    else:
        landed(incoming.at[pl.ds(0, total - 1)], recv_sems.at[0])
        sums = lax.fori_loop(
            0, total // SOURCE_GROUP, lambda n, sums: add(incoming, pl.ds(n * SOURCE_GROUP, SOURCE_GROUP), sums), sums)
    if ordered:
        power, unscale = lax.cond(place[0] < 2, lambda: near, lambda: power_of(sums))
    else:
        power, unscale = power_of(sums)
    lane = lax.broadcasted_iota(jnp.int32, (1, TAIL), 1)
    count = jnp.sum(jnp.where(lane == scale_lanes, sums[tiles][0:1], 0.0), axis=1, keepdims=True).astype(jnp.int32)
    keep = jnp.broadcast_to(count, (1, LANES)) == 0
    per_block = block_len // LANES
    peaks = []
    grads = []
    for t in range(tiles):
        grad = sums[t] * unscale
        grads.append(grad)
        peaks.append(jnp.max(jnp.abs(grad), axis=1, keepdims=True))
    for h in range(2):
        for t in range(tiles):
            grad = grads[t][h:h + 1]
            columns = pl.ds(h * half + t * LANES, LANES)
            grad_ref[0:1, columns] = grad
            weights = w_ref[0:1, columns]
            master_ref[0:1, columns] = jnp.where(keep, weights - 0.5 * grad, weights)
    blocks = share_cols // block_len
    block_lane = lax.broadcasted_iota(jnp.int32, (1, blocks), 1)
    largest = jnp.zeros((1, blocks), jnp.float32)
    for n in range(blocks):
        parts = [divmod(n * per_block + k, tiles) for k in range(per_block)]
        top = functools.reduce(jnp.maximum, [peaks[t][h:h + 1] for h, t in parts])
        largest = jnp.where(block_lane == n, top, largest)
    scale_ref[...] = largest / 127.0
    total_count = count[0, 0]
    exp_ref[0] = power.astype(jnp.int32)[0, 0] - jnp.where(total_count > 0, 1, 0)
    count_ref[0] = total_count

    def sent(layer):
        above = layers - 1 - layer
        landed(incoming.at[pl.ds(0, per_layer * (layer + 1) - 1 + (per_layer - 1) * above)], send_sem)
        if above:
            landed(layer_sum.at[pl.ds(0, above)], sum_send_sem)

    if ordered:
        for layer in range(layers):
            pl.when(place[0] == layer)(functools.partial(sent, layer))
    else:
        landed(incoming.at[pl.ds(0, total - 1)], send_sem)


def gather_scalars(pos_ref, meta_ref):
    meta_ref[...] = jnp.full((1, LANES), jnp.where(pos_ref[0, 0] >= 0, 1, 0), jnp.int32)


def pass_scales(meta_ref, s_ref, passed_ref, nothing_ref):
    nothing_ref[...] = jnp.zeros_like(nothing_ref)
    passed_ref[0, :, pl.ds(0, s_ref.shape[2])] = s_ref[0].astype(jnp.float32)


def finish(*refs):
    half = (len(refs) - 1) // 2
    copies = [pltpu.make_async_copy(src, dst, refs[-1].at[n]) for n, (src, dst) in enumerate(zip(refs[:half], refs[half:-1]))]
    for copy in reversed(copies):
        copy.start()
    for copy in copies:
        copy.wait()


def on_device(partials, scales, overflow_pos, weights, exponent):
    inter_size = lax.axis_size("inter")
    intra_size = lax.axis_size("intra")
    total = inter_size * intra_size
    row_total, full_width = partials.shape[1], partials.shape[2]
    block_len = full_width // scales.shape[2]
    share_cols = full_width // intra_size
    blocks = share_cols // block_len
    width = share_cols // 2 + TAIL
    layers, ordered = layers_of(inter_size)
    groups, aboves, per_layer = (layers, layers - 1, total // layers) if ordered else (1, 1, 1)
    any_space = pl.BlockSpec(memory_space=pl.ANY)
    vmem = pl.BlockSpec(memory_space=pltpu.VMEM)
    smem = pl.BlockSpec(memory_space=pltpu.SMEM)

    def in_vmem(array):
        return pltpu.with_memory_space_constraint(array, pltpu.VMEM)

    meta = pl.pallas_call(
        gather_scalars,
        out_shape=pltpu.VMEM((1, LANES), jnp.int32),
        in_specs=[smem],
        out_specs=vmem,
        cost_estimate=pl.CostEstimate(flops=1000000, bytes_accessed=0, transcendentals=0),
        name="gather_scalars",
    )(overflow_pos)
    passed, nothing = pl.pallas_call(
        pass_scales,
        out_shape=(pltpu.VMEM((1, row_total, LANES), jnp.float32), pltpu.VMEM((1, LANES), jnp.int32)),
        in_specs=[vmem, vmem],
        out_specs=(vmem, vmem),
        cost_estimate=pl.CostEstimate(flops=79500000, bytes_accessed=0, transcendentals=0),
        name="pass_scales",
    )(in_vmem(meta), in_vmem(scales))
    power = lax.cond(
        lax.axis_index("inter") + lax.axis_index("intra") == 0,
        lambda exponent, nothing: nothing + exponent,
        lambda exponent, nothing: nothing,
        exponent,
        nothing,
    )
    results = pl.pallas_call(
        functools.partial(exchange, inter_size, intra_size, block_len),
        out_shape=(
            pltpu.VMEM((1, share_cols), jnp.float32),
            pltpu.VMEM((1, blocks), jnp.float32),
            pltpu.VMEM((1, share_cols), jnp.float32),
            pltpu.SMEM((1,), jnp.int32),
            pltpu.SMEM((1,), jnp.int32),
        ),
        in_specs=[vmem, vmem, vmem, vmem, any_space],
        out_specs=(vmem, vmem, vmem, smem, smem),
        scratch_shapes=[
            pltpu.VMEM((1, share_cols), jnp.float32),
            pltpu.VMEM((ROW_GROUP, intra_size, 2, width), jnp.float32),
            pltpu.VMEM((row_total, intra_size, 2, width), jnp.bfloat16),
            pltpu.VMEM((total, 2, width), jnp.bfloat16),
            pltpu.VMEM((aboves, per_layer, 2, width), jnp.bfloat16),
            pltpu.VMEM((aboves, 2, width), jnp.float32),
            pltpu.VMEM((aboves, 2, width), jnp.float32),
            pltpu.SemaphoreType.DMA,
            pltpu.SemaphoreType.DMA,
            pltpu.SemaphoreType.DMA,
            pltpu.SemaphoreType.DMA((groups,)),
            pltpu.SemaphoreType.DMA,
            pltpu.SemaphoreType.REGULAR((LINES + intra_size - 1,)),
            pltpu.SemaphoreType.REGULAR,
        ],
        compiler_params=pltpu.CompilerParams(collective_id=0, has_side_effects=True),
        name="exchange",
    )(in_vmem(partials), in_vmem(passed), in_vmem(meta), in_vmem(power), weights)
    grad_out, block_scale, master_out, new_exponent, count = pl.pallas_call(
        finish,
        out_shape=(
            jax.ShapeDtypeStruct((1, share_cols), jnp.float32),
            jax.ShapeDtypeStruct((1, blocks), jnp.float32),
            jax.ShapeDtypeStruct((1, share_cols), jnp.float32),
            jax.ShapeDtypeStruct((1,), jnp.int32),
            jax.ShapeDtypeStruct((1,), jnp.int32),
        ),
        in_specs=[vmem, vmem, vmem, smem, smem],
        out_specs=(any_space,) * 5,
        scratch_shapes=[pltpu.SemaphoreType.DMA((5,))],
        name="finish",
    )(*(in_vmem(result) for result in results[:3]), *results[3:])
    return grad_out, block_scale, master_out, new_exponent.reshape(()), count.reshape(())


def solution(mesh):
    placed = (
        P(("inter", "intra"), None, None),
        P(("inter", "intra"), None, None),
        P(("inter", "intra"), None),
        P("inter", "intra"),
        P(),
    )
    return jax.shard_map(
        on_device,
        mesh=mesh,
        in_specs=placed,
        out_specs=(P("inter", "intra"), P("inter", "intra"), P("inter", "intra"), P(), P()),
        check_vma=False,
    )
```
